32 devices in a mesh: seq: 8 (over z, x), head: 4 (over y, core).
Axes of the slice: x: 2, y: 2, z: 4, core: 2. Of those that a mesh axis runs over, the one named last changes fastest.
Arguments:
- q_latent: bfloat16 [2048, 1536], P('seq', 'head'), may hold values from -6 to 6
- kv_latent: bfloat16 [2048, 512], P('seq', 'head'), may hold values from -6 to 6
- k_rope: bfloat16 [2048, 64], P('seq'), may hold values from -6 to 6
- segment_ids: int32 [2048], P('seq'), may hold values from 0 to 7, as said below
- w_q_nope: bfloat16 [1536, 16384], P('seq', 'head'), may hold values from -6 to 6
- w_q_rope: bfloat16 [1536, 8192], P('seq', 'head'), may hold values from -6 to 6
- w_kv_nope: bfloat16 [512, 16384], P('seq', 'head'), may hold values from -6 to 6
- threshold: float32 [1], replicated, may hold values from 3.5 to 5.5
Outputs:
- new_q_nope: bfloat16 [1536, 16384], P('seq', 'head')
- new_q_rope: bfloat16 [1536, 8192], P('seq', 'head')
- new_kv_nope: bfloat16 [512, 16384], P('seq', 'head')
- head_max: float32 [128], P('head')
- row_max: float32 [2048, 128], P('seq', 'head')
The draws below stay inside these ranges and needn't reach their ends.
Inputs may be any that keep to these rules, and one draw needn't show every extreme that they name: segment_ids never fall along the tokens and each document has 1 to 768 tokens.
All inputs are finite; a program needn't handle non-finite values.
Results may differ from the reference program's by a relative error of at most 0.0034.
Values may be sent and summed in bfloat16 or wider, within the bound.
A program may use at most 128 MiB of HBM per device.

```python
import math
import jax
import jax.numpy as jnp
from jax import lax

H = 128
D_NOPE = 128
D_ROPE = 64
QLORA = 1536
KVLORA = 512
TOK_DEV = 256
REACH = 3
TOKENS = 2048
N_SEQ = 8


def draw_segment_ids(key, part):
    count_blocks = TOKENS // TOK_DEV
    offsets = jax.random.randint(jax.random.fold_in(key, 11), (count_blocks,), 1, TOK_DEV - 1)
    position = jnp.arange(TOKENS, dtype=jnp.int32)
    block = position // TOK_DEV
    within = position % TOK_DEV
    regular = (within == offsets[block]) & (block <= count_blocks - 4)
    long_start = (count_blocks - 3) * TOK_DEV - 1
    flags = regular | (position == 0) | (position == long_start) | (position == TOKENS - 1)
    return (jnp.cumsum(flags.astype(jnp.int32)) - 1).astype(jnp.int32)


def block_scale(stream_key, shape, pieces, low, top_value):
    level, own = 1.0, jax.random.fold_in(stream_key, 6)
    for dim, parts in pieces:
        heights = jnp.exp(jax.random.uniform(jax.random.fold_in(own, dim), (parts,), jnp.float32, low / len(pieces), top_value / len(pieces)))
        level = level * jnp.repeat(heights, shape[dim] // parts).reshape([-1 if axis == dim else 1 for axis in range(len(shape))])
    return level


def gaussian(own_key, shape, scale, bound, split=(), kind=jnp.bfloat16):
    entries = jax.random.normal(own_key, shape, jnp.float32) * scale
    if len(split) > 0:
        entries = block_scale(own_key, shape, split, -0.22, 0.18) * entries
    return jnp.clip(entries, min=-bound, max=bound).astype(kind)


def setup_inputs(seed: int = 0) -> dict:
    key_list = jax.random.split(jax.random.key(seed), 9)
    q_latent = gaussian(key_list[0], (TOKENS, QLORA), 1.0, 6.0, ((0, 8), (1, 4)))
    kv_latent = gaussian(key_list[1], (TOKENS, KVLORA), 1.0, 6.0, ((0, 8), (1, 4)))
    k_rope = gaussian(key_list[2], (TOKENS, D_ROPE), 1.0, 6.0, ((0, 8),))
    segment_ids = draw_segment_ids(jax.random.fold_in(key_list[8], 71), 0)
    w_q_nope = gaussian(key_list[4], (QLORA, H * D_NOPE), 1.0, 6.0, ((0, 8), (1, 4)))
    w_q_rope = gaussian(key_list[5], (QLORA, H * D_ROPE), 1.0, 6.0, ((0, 8), (1, 4)))
    w_kv_nope = gaussian(key_list[6], (KVLORA, H * D_NOPE), 1.0, 6.0, ((0, 8), (1, 4)))
    threshold = jnp.clip(jax.random.uniform(key_list[7], (1,), jnp.float32, 3.5, 5.5), 3.5, 5.5)
    return dict(q_latent=q_latent, kv_latent=kv_latent, k_rope=k_rope, segment_ids=segment_ids, w_q_nope=w_q_nope, w_q_rope=w_q_rope, w_kv_nope=w_kv_nope, threshold=threshold)


def reference(q_latent, kv_latent, k_rope, segment_ids, w_q_nope, w_q_rope, w_kv_nope, threshold):
    q_scale = 1.0 / math.sqrt(QLORA)
    k_scale = 1.0 / math.sqrt(KVLORA)
    score_scale = 1.0 / math.sqrt(D_NOPE + D_ROPE)
    window = (REACH + 1) * TOK_DEV

    def advance(carry, block):
        old_nope, old_rope, old_seg = carry
        start = (block * TOK_DEV).astype(jnp.int32)
        q_lat = lax.dynamic_slice_in_dim(q_latent, start, TOK_DEV, 0)
        kv_lat = lax.dynamic_slice_in_dim(kv_latent, start, TOK_DEV, 0)
        rope_own = lax.dynamic_slice_in_dim(k_rope, start, TOK_DEV, 0)
        seg_own = lax.dynamic_slice_in_dim(segment_ids, start, TOK_DEV, 0)
        query_nope = (jnp.dot(q_lat, w_q_nope, preferred_element_type=jnp.float32) * q_scale).astype(jnp.bfloat16).reshape(TOK_DEV, H, D_NOPE)
        query_rope = (jnp.dot(q_lat, w_q_rope, preferred_element_type=jnp.float32) * q_scale).astype(jnp.bfloat16).reshape(TOK_DEV, H, D_ROPE)
        key_own = (jnp.dot(kv_lat, w_kv_nope, preferred_element_type=jnp.float32) * k_scale).astype(jnp.bfloat16)
        all_nope = jnp.concatenate([old_nope, key_own[None]], 0)
        all_rope = jnp.concatenate([old_rope, rope_own[None]], 0)
        all_seg = jnp.concatenate([old_seg, seg_own[None]], 0)
        keys_nope = all_nope.reshape(window, H, D_NOPE)
        keys_rope = all_rope.reshape(window, D_ROPE)
        keys_seg = all_seg.reshape(window)
        query_pos = start + jnp.arange(TOK_DEV, dtype=jnp.int32)
        key_pos = start - REACH * TOK_DEV + jnp.arange(window, dtype=jnp.int32)
        allowed = (seg_own[:, None] == keys_seg[None, :]) & (key_pos[None, :] <= query_pos[:, None]) & (key_pos[None, :] >= 0)
        nope = jnp.einsum('qhd,khd->hqk', query_nope.astype(jnp.float32), keys_nope.astype(jnp.float32))
        rope = jnp.einsum('qhd,kd->hqk', query_rope.astype(jnp.float32), keys_rope.astype(jnp.float32))
        scores = (nope + rope) * score_scale
        block_rows = lax.optimization_barrier(jnp.max(jnp.where(allowed[None], scores, jnp.float32(-1e+30)), axis=2))
        return ((all_nope[1:], all_rope[1:], all_seg[1:]), block_rows.T)
    init = (jnp.zeros((REACH, TOK_DEV, H * D_NOPE), jnp.bfloat16), jnp.zeros((REACH, TOK_DEV, D_ROPE), jnp.bfloat16), jnp.zeros((REACH, TOK_DEV), jnp.int32))
    carry, rows = lax.scan(advance, init, jnp.arange(N_SEQ, dtype=jnp.int32))
    row_max = rows.reshape(TOKENS, H)
    head_max = lax.optimization_barrier(jnp.max(row_max, axis=0))
    clip = threshold[0] / jnp.maximum(head_max, threshold[0])
    root = jnp.sqrt(clip)
    new_q_nope = (w_q_nope.astype(jnp.float32) * jnp.repeat(root, D_NOPE)[None, :]).astype(jnp.bfloat16)
    new_q_rope = (w_q_rope.astype(jnp.float32) * jnp.repeat(clip, D_ROPE)[None, :]).astype(jnp.bfloat16)
    new_kv_nope = (w_kv_nope.astype(jnp.float32) * jnp.repeat(root, D_NOPE)[None, :]).astype(jnp.bfloat16)
    return (new_q_nope, new_q_rope, new_kv_nope, head_max, row_max)
```

```python
import functools
import math

import jax
import jax.numpy as jnp
from jax import lax
from jax.experimental import pallas as pl
from jax.experimental.pallas import tpu as pltpu
from jax.sharding import PartitionSpec as P

D_NOPE = 128
D_ROPE = 64
QLORA = 1536
KVLORA = 512
REACH = 3


def as_sent(value):
    return jax.tree.map(lambda a: a.astype(jnp.bfloat16) if a.dtype == jnp.float32 else a, value)


def from_partner(value, axis, stride):
    mask = 2**stride
    pairs = [(source, source ^ mask) for source in range(lax.axis_size(axis))]
    return lax.ppermute(value, axis, pairs)


def shifted(block, axis, distance):
    devices = range(lax.axis_size(axis))
    route = [(i - distance, i) for i in devices if i - distance in devices]
    return lax.ppermute(block, axis, route)


def score_max(query_nope, query_rope, key_nope, key_rope, allowed):
    nope = jnp.einsum("qhd,khd->hqk", query_nope, key_nope, preferred_element_type=jnp.float32)
    rope = jnp.einsum("qhd,kd->hqk", query_rope, key_rope, preferred_element_type=jnp.float32)
    scores = (nope + rope) * (1.0 / math.sqrt(D_NOPE + D_ROPE))
    return jnp.max(jnp.where(allowed[None], scores, jnp.float32(-1e30)), axis=2)


def masked_max(compute, operands):
    return compute(*operands)


def spread_columns(weight, width, quarter, copies):
    pieces = weight.reshape(weight.shape[0], 4, quarter * width).transpose(1, 0, 2)
    return jnp.tile(pieces, (copies, 1, 1))


def grouped_body(q_latent, kv_latent, k_rope, segment_ids, w_q_nope, w_q_rope, w_kv_nope, threshold):
    q_whole, kv_whole = (
        lax.all_gather(q_latent, "head", axis=1, tiled=True),
        lax.all_gather(kv_latent, "head", axis=1, tiled=True),
    )
    rows = q_whole.shape[0]
    heads = w_q_nope.shape[1] // D_NOPE
    q_scale = 1.0 / math.sqrt(QLORA)
    k_scale = 1.0 / math.sqrt(KVLORA)
    place = lax.axis_index("seq")
    quarter = heads // 4
    copies = lax.axis_size("seq") // 4
    slot = place % 4
    sent = (
        spread_columns(w_q_nope, D_NOPE, quarter, copies),
        spread_columns(w_q_rope, D_ROPE, quarter, copies),
        spread_columns(w_kv_nope, D_NOPE, quarter, copies),
    )
    got_nope, got_rope, got_kv = (
        lax.all_to_all(sent[0], "seq", split_axis=0, concat_axis=1, tiled=True),
        lax.all_to_all(sent[1], "seq", split_axis=0, concat_axis=1, tiled=True),
        lax.all_to_all(sent[2], "seq", split_axis=0, concat_axis=1, tiled=True),
    )
    sub_nope = got_nope.reshape(QLORA, quarter * D_NOPE)
    sub_rope = got_rope.reshape(QLORA, quarter * D_ROPE)
    sub_kv = got_kv.reshape(KVLORA, quarter * D_NOPE)
    group = (q_whole, kv_whole, k_rope)
    for level in range(2):
        partner = jax.tree.map(
            lambda part, own: part.astype(own.dtype),
            from_partner(as_sent(group), "seq", level),
            group,
        )
        upper = place // (1 << level) % 2 == 1
        group = tuple(
            (
                jnp.where(
                    upper, jnp.concatenate([other, mine], 0), jnp.concatenate([mine, other], 0)
                )
                for mine, other in zip(group, partner)
            )
        )
    group_q, group_kv, group_rope = group
    early_kv, early_rope = shifted(
        (group_kv[(4 - REACH) * rows :], group_rope[(4 - REACH) * rows :]), "seq", 4
    )
    keys_kv = jnp.concatenate([early_kv, group_kv], 0)
    keys_rope = jnp.concatenate([early_rope, group_rope], 0)
    key_nope = (
        (jnp.dot(keys_kv, sub_kv, preferred_element_type=jnp.float32) * k_scale)
        .astype(jnp.bfloat16)
        .reshape(keys_kv.shape[0], quarter, D_NOPE)
    )
    query_nope = (
        (jnp.dot(group_q, sub_nope, preferred_element_type=jnp.float32) * q_scale)
        .astype(jnp.bfloat16)
        .reshape(4 * rows, quarter, D_NOPE)
    )
    query_rope = (
        (jnp.dot(group_q, sub_rope, preferred_element_type=jnp.float32) * q_scale)
        .astype(jnp.bfloat16)
        .reshape(4 * rows, quarter, D_ROPE)
    )
    all_segs = lax.all_gather(segment_ids, "seq", axis=0, tiled=True)
    padded_segs = jnp.concatenate([jnp.full((REACH * rows,), -1, jnp.int32), all_segs], 0)
    first = place // 4 * 4
    window = (REACH + 1) * rows
    block_rows = []
    for local in range(4):
        block = first + local
        query_seg = lax.dynamic_slice_in_dim(all_segs, block * rows, rows, 0)
        key_seg = lax.dynamic_slice_in_dim(padded_segs, block * rows, window, 0)
        query_pos = block * rows + jnp.arange(rows, dtype=jnp.int32)
        key_pos = (block - REACH) * rows + jnp.arange(window, dtype=jnp.int32)
        allowed = (
            (query_seg[:, None] == key_seg[None, :])
            & (key_pos[None, :] <= query_pos[:, None])
            & (key_pos[None, :] >= 0)
        )
        operands = (
            query_nope[local * rows : (local + 1) * rows],
            query_rope[local * rows : (local + 1) * rows],
            key_nope[local * rows : local * rows + window],
            keys_rope[local * rows : local * rows + window],
            allowed,
        )
        block_rows.append(masked_max(score_max, operands))
    stacked = jnp.stack(block_rows, 0)[None]
    for level in range(2):
        partner = from_partner(stacked, "seq", level)
        upper = place // (1 << level) % 2 == 1
        stacked = jnp.where(
            upper, jnp.concatenate([partner, stacked], 0), jnp.concatenate([stacked, partner], 0)
        )
    own = lax.dynamic_index_in_dim(stacked, slot, 1, False)
    row_max = own.reshape(heads, rows).T
    local_heads = jnp.max(row_max, axis=0)
    head_max = lax.pmax(local_heads, "seq")
    return finish(threshold, head_max, row_max, w_q_nope, w_q_rope, w_kv_nope)


def finish(threshold, head_max, row_max, w_q_nope, w_q_rope, w_kv_nope):
    clip = threshold[0] / jnp.maximum(head_max, threshold[0])
    root = jnp.sqrt(clip)
    new_q_nope = (w_q_nope.astype(jnp.float32) * jnp.repeat(root, D_NOPE)[None, :]).astype(
        jnp.bfloat16
    )
    new_q_rope = (w_q_rope.astype(jnp.float32) * jnp.repeat(clip, D_ROPE)[None, :]).astype(
        jnp.bfloat16
    )
    new_kv_nope = (w_kv_nope.astype(jnp.float32) * jnp.repeat(root, D_NOPE)[None, :]).astype(
        jnp.bfloat16
    )
    return (new_q_nope, new_q_rope, new_kv_nope, head_max, row_max)


MESH = pl.DeviceIdType.MESH
LANES = 128


def other(index, stride):
    return index + stride - 2 * stride * (index // stride % 2)


def flip(index, bits):
    stride = 1
    while stride <= bits:
        if bits & stride:
            index = other(index, stride)
        stride *= 2
    return index


def halvings(size):
    return [size >> (i + 1) for i in range(size.bit_length() - 1)]


def layer_kernel(
    n, m, own, q_lat, kv_lat, rope, segs, w_nope, w_rope, w_kv, got,
    q_all, kv_all, rope_all, segs_all, w_even, w_odd, w_key, keys, caps, seg_cols, pair_rope, near_sum, maxima,
    q_send, q_recv, kv_send, kv_recv, rope_send, rope_recv, seg_send, seg_recv, w_send, w_recv, max_send, max_recv, local,
):
    s = lax.axis_index("seq")
    h = lax.axis_index("head")
    rows = q_lat.shape[0]
    part = rope.shape[0] // m
    pairs = own // 2
    q_rows = w_nope.shape[0]
    kv_rows = w_kv.shape[0]
    half = n // 2
    routes = [("seq", stride) for stride in halvings(n)] + [("head", stride) for stride in halvings(m)]
    last = len([1 for axis, _ in routes if axis == "seq"])

    barrier = pltpu.get_barrier_semaphore()
    for k in range(1, n):
        pl.semaphore_signal(barrier, inc=1, device_id=(flip(s, k), h), device_id_type=MESH)
    for stride in halvings(m):
        pl.semaphore_signal(barrier, inc=1, device_id=(s, other(h, stride)), device_id_type=MESH)

    def window(whole, width, ps, ph):
        return whole.at[pl.ds(pl.multiple_of(ps * rows, rows), rows), pl.ds(pl.multiple_of(ph * width, LANES), width)]

    def places(k, g):
        ps, ph = flip(s, k), flip(h, g)
        return (
            window(q_all, q_lat.shape[1], ps, ph),
            window(kv_all, kv_lat.shape[1], ps, ph),
            rope_all.at[ps, pl.ds(pl.multiple_of(ph * part, part), part), :],
        )

    def parts_of(p):
        found = []
        for j in range(pairs):
            even = pl.ds(pl.multiple_of((p * own + 2 * j) * LANES, LANES), LANES)
            odd = pl.ds(pl.multiple_of((p * own + 2 * j + 1) * LANES, LANES), LANES)
            both = pl.ds(pl.multiple_of((p * pairs + j) * LANES, LANES), LANES)
            found.append((w_nope.at[:, even], w_even, j, slice(0, LANES)))
            found.append((w_rope.at[:, both], w_even, j, slice(LANES, 2 * LANES)))
            found.append((w_nope.at[:, odd], w_odd, j, slice(0, LANES)))
        found.append((w_kv.at[:, pl.ds(pl.multiple_of(p * own * LANES, LANES), own * LANES)], w_key, None, None))
        return found

    def landing(target, j, columns, source):
        if j is None:
            return target.at[pl.ds(pl.multiple_of(source * kv_rows, kv_rows), kv_rows), :]
        return target.at[j, pl.ds(pl.multiple_of(source * q_rows, q_rows), q_rows), columns]

    own_pieces = (q_lat, kv_lat, rope.at[pl.ds(pl.multiple_of(h * part, part), part), :], segs)
    loads = [
        pltpu.make_async_copy(src, dst, local.at[i])
        for i, (src, dst) in enumerate(zip(own_pieces, places(0, 0) + (segs_all.at[s],)))
    ]
    for copy in loads:
        copy.start()
    keeps = [
        pltpu.make_async_copy(src, landing(target, j, columns, s), local.at[4 + i])
        for i, (src, target, j, columns) in enumerate(parts_of(s))
    ]
    for copy in keeps:
        copy.start()
    pl.semaphore_wait(barrier, n - 1 + len(halvings(m)))
    for copy in loads:
        copy.wait()

    drains = []
    slots = [0]

    def push(k, g, route):
        axis, stride = route
        target = (other(s, stride), h) if axis == "seq" else (s, other(h, stride))
        at = (k ^ stride) * m + g if axis == "seq" else k * m + (g ^ stride)
        slot = slots[0]
        slots[0] += 1
        for ref, sent, taken in zip(places(k, g), (q_send, kv_send, rope_send), (q_recv, kv_recv, rope_recv)):
            copy = pltpu.make_async_remote_copy(
                src_ref=ref, dst_ref=ref, send_sem=sent.at[slot], recv_sem=taken.at[at],
                device_id=target, device_id_type=MESH)
            copy.start()
            drains.append((ref, sent.at[slot]))

    def relay(k, g):
        for ref, taken in zip(places(k, g), (q_recv, kv_recv, rope_recv)):
            pltpu.make_async_copy(ref, ref, taken.at[k * m + g]).wait()
        reached = max(i for i, (axis, stride) in enumerate(routes) if (k if axis == "seq" else g) & stride)
        for route in routes[reached + 1:]:
            push(k, g, route)

    def weights(wanted, k):
        p = flip(s, k)
        for i, (src, target, j, columns) in enumerate(parts_of(p)):
            if i in wanted:
                copy = pltpu.make_async_remote_copy(
                    src_ref=src, dst_ref=landing(target, j, columns, s),
                    send_sem=w_send.at[i * n + k], recv_sem=w_recv.at[i * n + k],
                    device_id=(p, h), device_id_type=MESH)
                copy.start()
                drains.append((src, w_send.at[i * n + k]))

    def take(wanted, ks):
        for k in ks:
            for i, (_, target, j, columns) in enumerate(parts_of(s)):
                if i in wanted:
                    ref = landing(target, j, columns, flip(s, k))
                    pltpu.make_async_copy(ref, ref, w_recv.at[i * n + k]).wait()

    far = [k ^ half for k in range(half)]
    near = list(range(half - 1, 0, -1))
    kv_part = 3 * pairs
    first = [0, 1]
    later = [[kv_part]] + [[2]] + [group for j in range(1, pairs) for group in ([3 * j, 3 * j + 1], [3 * j + 2])]

    for route in routes:
        push(0, 0, route)
    for k in range(1, n):
        copy = pltpu.make_async_remote_copy(
            src_ref=segs_all.at[s], dst_ref=segs_all.at[s], send_sem=seg_send.at[k], recv_sem=seg_recv.at[k],
            device_id=(flip(s, k), h), device_id_type=MESH)
        copy.start()
        drains.append((segs_all.at[s], seg_send.at[k]))
    for k in far:
        weights(first, k)
    order = sorted(range(1, n), key=lambda k: (bin(k).count("1"), k & 1 == 1 and bin(k).count("1") > 1, k))
    on_links = max(i for i, k in enumerate(order) if k & 1 == 0)
    for k in order[: on_links + 1]:
        relay(k, 0)
    for k in near:
        weights(first, k)
    for wanted in later:
        for k in far + near:
            weights(wanted, k)

    for k in range(1, n):
        ref = segs_all.at[flip(s, k)]
        pltpu.make_async_copy(ref, ref, seg_recv.at[k]).wait()

    def fill_segs(block, carry):
        here = pl.ds(pl.multiple_of(block * rows, rows), rows)
        seg_cols[here, :] = jnp.transpose(jnp.broadcast_to(segs_all[block], (LANES, rows)))
        return carry

    lax.fori_loop(0, n, fill_segs, 0)
    reach = (REACH + 1) * rows

    def range_of(block):
        start = jnp.maximum(block - REACH, 0) * rows
        return start, pl.ds(pl.multiple_of(start, rows), reach)

    def fill_caps(block, carry):
        start, span = range_of(block)
        key_segs = jnp.concatenate([seg_cols[span, :]] * (rows // LANES), 1)
        key_pos = start + lax.broadcasted_iota(jnp.int32, (reach, rows), 0)
        query_pos = block * rows + lax.broadcasted_iota(jnp.int32, (reach, rows), 1)
        allowed = (key_segs == segs_all[block]) & (key_pos <= query_pos)
        caps[block] = jnp.where(allowed, jnp.float32(3.4e38), jnp.float32(-1e30))
        return carry

    lax.fori_loop(0, n, fill_caps, 0)

    for k in order[on_links + 1:]:
        relay(k, 0)
    for g in range(1, m):
        for k in [0] + order:
            relay(k, g)

    for copy in keeps:
        copy.wait()
    take([kv_part], far + near)
    q_scale = 1.0 / math.sqrt(QLORA)
    k_scale = 1.0 / math.sqrt(KVLORA)
    lane = lax.broadcasted_iota(jnp.int32, (rows, LANES), 1)
    sides = LANES // D_ROPE

    def fill_keys(block, carry):
        here = pl.ds(pl.multiple_of(block * rows, rows), rows)
        key = (jnp.dot(kv_all[here, :], w_key[...], preferred_element_type=jnp.float32) * k_scale).astype(jnp.bfloat16)
        turned = jnp.concatenate([rope_all[block].astype(jnp.float32)] * sides, 0)
        twice = jnp.transpose(turned).astype(jnp.bfloat16)
        for i in range(own):
            side = jnp.where(lane // D_ROPE == i % sides, twice, jnp.zeros_like(twice))
            keys[i, here, :] = jnp.concatenate([key[:, i * D_NOPE : (i + 1) * D_NOPE], side], 1)
        return carry

    lax.fori_loop(0, n, fill_keys, 0)

    def top_logits(i, block, q_head):
        here = pl.ds(pl.multiple_of(block * rows, rows), rows)
        _, span = range_of(block)
        logits = lax.dot_general(
            keys[i, span, :], q_head, (((1,), (1,)), ((), ())), preferred_element_type=jnp.float32
        )
        top = jnp.max(jnp.minimum(logits, caps[block]), axis=0, keepdims=True)
        maxima[i : i + 1, here] = top * (1.0 / math.sqrt(D_NOPE + D_ROPE))

    depth = half * q_rows
    close = pl.multiple_of(s // half * depth, depth)
    distant = pl.multiple_of((1 - s // half) * depth, depth)

    for j in range(pairs):
        take([3 * j, 3 * j + 1], far + near)

        def even_head(block, carry):
            here = pl.ds(pl.multiple_of(block * rows, rows), rows)
            query = jnp.dot(q_all[here, :], w_even[j], preferred_element_type=jnp.float32)
            query = (query * q_scale).astype(jnp.bfloat16)
            pair_rope[here, :] = query[:, LANES:]
            top_logits(2 * j, block, query)
            return carry

        lax.fori_loop(0, n, even_head, 0)
        take([3 * j + 2], near)

        def odd_near(block, carry):
            here = pl.ds(pl.multiple_of(block * rows, rows), rows)
            near_sum[here, :] = jnp.dot(
                q_all[here, pl.ds(close, depth)], w_odd[j, pl.ds(close, depth), :], preferred_element_type=jnp.float32
            )
            return carry

        lax.fori_loop(0, n, odd_near, 0)
        take([3 * j + 2], far)

        def odd_head(block, carry):
            here = pl.ds(pl.multiple_of(block * rows, rows), rows)
            query = near_sum[here, :] + jnp.dot(
                q_all[here, pl.ds(distant, depth)], w_odd[j, pl.ds(distant, depth), :], preferred_element_type=jnp.float32
            )
            query = (query * q_scale).astype(jnp.bfloat16)
            top_logits(2 * j + 1, block, jnp.concatenate([query, pair_rope[here, :]], 1))
            return carry

        lax.fori_loop(0, n, odd_head, 0)

    best = jnp.max(maxima[0:own, :], axis=1, keepdims=True)
    maxima[own : 2 * own, :] = jnp.broadcast_to(best, (own, maxima.shape[1]))
    shares = []
    for k in range(1, n):
        p = flip(s, k)
        copy = pltpu.make_async_remote_copy(
            src_ref=maxima.at[:, pl.ds(pl.multiple_of(p * rows, rows), rows)], dst_ref=got.at[s],
            send_sem=max_send.at[k], recv_sem=max_recv.at[k], device_id=(p, h), device_id_type=MESH)
        copy.start()
        shares.append(copy)
    got[s] = maxima[:, pl.ds(pl.multiple_of(s * rows, rows), rows)]
    for ref, sent in drains:
        pltpu.make_async_copy(ref, ref, sent).wait()
    for k, copy in zip(range(1, n), shares):
        copy.wait_send()
        at = got.at[flip(s, k)]
        pltpu.make_async_copy(at, at, max_recv.at[k]).wait()


def layer(n, m, own, q_lat, kv_lat, rope, segs, w_nope, w_rope, w_kv):
    rows = q_lat.shape[0]
    tokens = n * rows
    pairs = own // 2
    moves = n * m - 1
    parts = 3 * pairs + 1
    any_ref = pl.BlockSpec(memory_space=pl.ANY)
    dma = pltpu.SemaphoreType.DMA
    kind = q_lat.dtype
    return pl.pallas_call(
        functools.partial(layer_kernel, n, m, own),
        out_shape=jax.ShapeDtypeStruct((n, 2 * own, rows), jnp.float32),
        in_specs=[any_ref] * 7,
        out_specs=pl.BlockSpec(memory_space=pltpu.VMEM),
        scratch_shapes=[
            pltpu.VMEM((tokens, m * q_lat.shape[1]), kind),
            pltpu.VMEM((tokens, m * kv_lat.shape[1]), kind),
            pltpu.VMEM((n,) + rope.shape, kind),
            pltpu.VMEM((n,) + segs.shape, jnp.int32),
            pltpu.VMEM((pairs, n * w_nope.shape[0], 2 * LANES), kind),
            pltpu.VMEM((pairs, n * w_nope.shape[0], LANES), kind),
            pltpu.VMEM((n * w_kv.shape[0], own * LANES), kind),
            pltpu.VMEM((own, tokens, D_NOPE + LANES), kind),
            pltpu.VMEM((n, (REACH + 1) * rows, rows), jnp.float32),
            pltpu.VMEM((tokens, LANES), jnp.int32),
            pltpu.VMEM((tokens, LANES), kind),
            pltpu.VMEM((tokens, LANES), jnp.float32),
            pltpu.VMEM((2 * own, tokens), jnp.float32),
            dma((moves,)), dma((n * m,)), dma((moves,)), dma((n * m,)), dma((moves,)), dma((n * m,)),
            dma((n,)), dma((n,)),
            dma((parts * n,)), dma((parts * n,)), dma((n,)), dma((n,)), dma((4 + parts,)),
        ],
        compiler_params=pltpu.CompilerParams(
            collective_id=0, has_side_effects=True, vmem_limit_bytes=44 * 1024 * 1024
        ),
        name="layer",
    )(q_lat, kv_lat, rope, segs, w_nope, w_rope, w_kv)


def clip_kernel(n, own, got, threshold, w_nope, w_rope, w_kv, new_nope, new_rope, new_kv, head_max, row_max):
    limit = threshold[0]
    lane = lax.broadcasted_iota(jnp.int32, (1, LANES), 1)
    tops = jnp.zeros((1, head_max.shape[1]), jnp.float32)
    place = lax.broadcasted_iota(jnp.int32, tops.shape, 1)

    def scaled(source, target, columns, factor):
        target[:, columns] = (source[:, columns].astype(jnp.float32) * factor).astype(target.dtype)

    for s in range(n):
        top = got[s, own : 2 * own, 0:LANES]
        clip = limit / jnp.maximum(top, limit)
        root = jnp.sqrt(clip)
        for i in range(own):
            head = s * own + i
            columns = slice(head * LANES, (head + 1) * LANES)
            scaled(w_nope, new_nope, columns, root[i : i + 1])
            scaled(w_kv, new_kv, columns, root[i : i + 1])
            tops = jnp.where(place == head, top[i : i + 1, 0 : tops.shape[1]], tops)
        for j in range(own // 2):
            pair = s * own // 2 + j
            columns = slice(pair * LANES, (pair + 1) * LANES)
            factor = jnp.where(lane < D_ROPE, clip[2 * j : 2 * j + 1], clip[2 * j + 1 : 2 * j + 2])
            scaled(w_rope, new_rope, columns, factor)
        row_max[s * own : (s + 1) * own, :] = got[s, 0:own, :]
    head_max[...] = tops


def clip_weights(n, own, got, threshold, w_nope, w_rope, w_kv):
    steps = 4 if w_nope.shape[0] % 64 == 0 and w_kv.shape[0] % 64 == 0 else 1
    weights = (w_nope, w_rope, w_kv)
    blocks = [pl.BlockSpec((w.shape[0] // steps, w.shape[1]), lambda i: (i, 0)) for w in weights]
    heads = n * own
    return pl.pallas_call(
        functools.partial(clip_kernel, n, own),
        grid=(steps,),
        out_shape=tuple(jax.ShapeDtypeStruct(w.shape, w.dtype) for w in weights)
        + (jax.ShapeDtypeStruct((1, heads), jnp.float32), jax.ShapeDtypeStruct((heads, got.shape[2]), jnp.float32)),
        in_specs=[pl.BlockSpec(got.shape, lambda i: (0, 0, 0)), pl.BlockSpec(memory_space=pltpu.SMEM)] + blocks,
        out_specs=tuple(blocks)
        + (pl.BlockSpec((1, heads), lambda i: (0, 0)), pl.BlockSpec((heads, got.shape[2]), lambda i: (0, 0))),
        compiler_params=pltpu.CompilerParams(dimension_semantics=("arbitrary",)),
        name="clip_weights",
    )(got, threshold, w_nope, w_rope, w_kv)


def owned_body(n, m, q_latent, kv_latent, k_rope, segment_ids, w_q_nope, w_q_rope, w_kv_nope, threshold):
    rows = q_latent.shape[0]
    heads = w_q_nope.shape[1] // D_NOPE
    own = heads // n
    got = layer(n, m, own, q_latent, kv_latent, k_rope.T, segment_ids.reshape(1, rows), w_q_nope, w_q_rope, w_kv_nope)
    new_nope, new_rope, new_kv, head_max, row_max = clip_weights(n, own, got, threshold, w_q_nope, w_q_rope, w_kv_nope)
    return (new_nope, new_rope, new_kv, head_max.reshape(heads), row_max.T)


def body(n, m, *operands):
    heads = operands[4].shape[1] // D_NOPE
    rows = operands[0].shape[0]
    shares = heads % n == 0 and heads // n % 4 == 0 and heads <= LANES
    powers = n & (n - 1) == 0 and m & (m - 1) == 0 and n > REACH
    small = n * rows * operands[0].shape[1] * m <= 2048 * 1536
    if shares and powers and small and rows % LANES == 0 and operands[2].shape[1] % (16 * m) == 0:
        return owned_body(n, m, *operands)
    return grouped_body(*operands)


def solution(mesh):
    in_specs = (
        P("seq", "head"),
        P("seq", "head"),
        P("seq", None),
        P("seq"),
        P("seq", "head"),
        P("seq", "head"),
        P("seq", "head"),
        P(),
    )
    out_specs = (P("seq", "head"), P("seq", "head"), P("seq", "head"), P("head"), P("seq", "head"))
    return jax.shard_map(functools.partial(body, mesh.shape["seq"], mesh.shape["head"]), mesh=mesh, in_specs=in_specs, out_specs=out_specs, check_vma=False)
```

```python
import functools
import math

import jax
import jax.numpy as jnp
from jax import lax
from jax.experimental import pallas as pl
from jax.experimental.pallas import tpu as pltpu
from jax.sharding import PartitionSpec as P

D_NOPE = 128
D_ROPE = 64
QLORA = 1536
KVLORA = 512
REACH = 3


def as_sent(value):
    return jax.tree.map(lambda a: a.astype(jnp.bfloat16) if a.dtype == jnp.float32 else a, value)


def from_partner(value, axis, stride):
    mask = 2**stride
    pairs = [(source, source ^ mask) for source in range(lax.axis_size(axis))]
    return lax.ppermute(value, axis, pairs)


def shifted(block, axis, distance):
    devices = range(lax.axis_size(axis))
    route = [(i - distance, i) for i in devices if i - distance in devices]
    return lax.ppermute(block, axis, route)


def score_max(query_nope, query_rope, key_nope, key_rope, allowed):
    nope = jnp.einsum("qhd,khd->hqk", query_nope, key_nope, preferred_element_type=jnp.float32)
    rope = jnp.einsum("qhd,kd->hqk", query_rope, key_rope, preferred_element_type=jnp.float32)
    scores = (nope + rope) * (1.0 / math.sqrt(D_NOPE + D_ROPE))
    return jnp.max(jnp.where(allowed[None], scores, jnp.float32(-1e30)), axis=2)


def masked_max(compute, operands):
    return compute(*operands)


def spread_columns(weight, width, quarter, copies):
    pieces = weight.reshape(weight.shape[0], 4, quarter * width).transpose(1, 0, 2)
    return jnp.tile(pieces, (copies, 1, 1))


def grouped_body(q_latent, kv_latent, k_rope, segment_ids, w_q_nope, w_q_rope, w_kv_nope, threshold):
    q_whole, kv_whole = (
        lax.all_gather(q_latent, "head", axis=1, tiled=True),
        lax.all_gather(kv_latent, "head", axis=1, tiled=True),
    )
    rows = q_whole.shape[0]
    heads = w_q_nope.shape[1] // D_NOPE
    q_scale = 1.0 / math.sqrt(QLORA)
    k_scale = 1.0 / math.sqrt(KVLORA)
    place = lax.axis_index("seq")
    quarter = heads // 4
    copies = lax.axis_size("seq") // 4
    slot = place % 4
    sent = (
        spread_columns(w_q_nope, D_NOPE, quarter, copies),
        spread_columns(w_q_rope, D_ROPE, quarter, copies),
        spread_columns(w_kv_nope, D_NOPE, quarter, copies),
    )
    got_nope, got_rope, got_kv = (
        lax.all_to_all(sent[0], "seq", split_axis=0, concat_axis=1, tiled=True),
        lax.all_to_all(sent[1], "seq", split_axis=0, concat_axis=1, tiled=True),
        lax.all_to_all(sent[2], "seq", split_axis=0, concat_axis=1, tiled=True),
    )
    sub_nope = got_nope.reshape(QLORA, quarter * D_NOPE)
    sub_rope = got_rope.reshape(QLORA, quarter * D_ROPE)
    sub_kv = got_kv.reshape(KVLORA, quarter * D_NOPE)
    group = (q_whole, kv_whole, k_rope)
    for level in range(2):
        partner = jax.tree.map(
            lambda part, own: part.astype(own.dtype),
            from_partner(as_sent(group), "seq", level),
            group,
        )
        upper = place // (1 << level) % 2 == 1
        group = tuple(
            (
                jnp.where(
                    upper, jnp.concatenate([other, mine], 0), jnp.concatenate([mine, other], 0)
                )
                for mine, other in zip(group, partner)
            )
        )
    group_q, group_kv, group_rope = group
    early_kv, early_rope = shifted(
        (group_kv[(4 - REACH) * rows :], group_rope[(4 - REACH) * rows :]), "seq", 4
    )
    keys_kv = jnp.concatenate([early_kv, group_kv], 0)
    keys_rope = jnp.concatenate([early_rope, group_rope], 0)
    key_nope = (
        (jnp.dot(keys_kv, sub_kv, preferred_element_type=jnp.float32) * k_scale)
        .astype(jnp.bfloat16)
        .reshape(keys_kv.shape[0], quarter, D_NOPE)
    )
    query_nope = (
        (jnp.dot(group_q, sub_nope, preferred_element_type=jnp.float32) * q_scale)
        .astype(jnp.bfloat16)
        .reshape(4 * rows, quarter, D_NOPE)
    )
    query_rope = (
        (jnp.dot(group_q, sub_rope, preferred_element_type=jnp.float32) * q_scale)
        .astype(jnp.bfloat16)
        .reshape(4 * rows, quarter, D_ROPE)
    )
    all_segs = lax.all_gather(segment_ids, "seq", axis=0, tiled=True)
    padded_segs = jnp.concatenate([jnp.full((REACH * rows,), -1, jnp.int32), all_segs], 0)
    first = place // 4 * 4
    window = (REACH + 1) * rows
    block_rows = []
    for local in range(4):
        block = first + local
        query_seg = lax.dynamic_slice_in_dim(all_segs, block * rows, rows, 0)
        key_seg = lax.dynamic_slice_in_dim(padded_segs, block * rows, window, 0)
        query_pos = block * rows + jnp.arange(rows, dtype=jnp.int32)
        key_pos = (block - REACH) * rows + jnp.arange(window, dtype=jnp.int32)
        allowed = (
            (query_seg[:, None] == key_seg[None, :])
            & (key_pos[None, :] <= query_pos[:, None])
            & (key_pos[None, :] >= 0)
        )
        operands = (
            query_nope[local * rows : (local + 1) * rows],
            query_rope[local * rows : (local + 1) * rows],
            key_nope[local * rows : local * rows + window],
            keys_rope[local * rows : local * rows + window],
            allowed,
        )
        block_rows.append(masked_max(score_max, operands))
    stacked = jnp.stack(block_rows, 0)[None]
    for level in range(2):
        partner = from_partner(stacked, "seq", level)
        upper = place // (1 << level) % 2 == 1
        stacked = jnp.where(
            upper, jnp.concatenate([partner, stacked], 0), jnp.concatenate([stacked, partner], 0)
        )
    own = lax.dynamic_index_in_dim(stacked, slot, 1, False)
    row_max = own.reshape(heads, rows).T
    local_heads = jnp.max(row_max, axis=0)
    head_max = lax.pmax(local_heads, "seq")
    return finish(threshold, head_max, row_max, w_q_nope, w_q_rope, w_kv_nope)


def finish(threshold, head_max, row_max, w_q_nope, w_q_rope, w_kv_nope):
    clip = threshold[0] / jnp.maximum(head_max, threshold[0])
    root = jnp.sqrt(clip)
    new_q_nope = (w_q_nope.astype(jnp.float32) * jnp.repeat(root, D_NOPE)[None, :]).astype(
        jnp.bfloat16
    )
    new_q_rope = (w_q_rope.astype(jnp.float32) * jnp.repeat(clip, D_ROPE)[None, :]).astype(
        jnp.bfloat16
    )
    new_kv_nope = (w_kv_nope.astype(jnp.float32) * jnp.repeat(root, D_NOPE)[None, :]).astype(
        jnp.bfloat16
    )
    return (new_q_nope, new_q_rope, new_kv_nope, head_max, row_max)


MESH = pl.DeviceIdType.MESH
LANES = 128


def other(index, stride):
    return index + stride - 2 * stride * (index // stride % 2)


def flip(index, bits):
    stride = 1
    while stride <= bits:
        if bits & stride:
            index = other(index, stride)
        stride *= 2
    return index


def halvings(size):
    return [size >> (i + 1) for i in range(size.bit_length() - 1)]


def layer_kernel(
    n, m, own, q_lat, kv_lat, rope, segs, w_nope, w_rope, w_kv, got, held_nope, held_rope, held_kv,
    q_all, kv_all, rope_all, segs_all, w_even, w_odd, w_key, keys, caps, seg_cols, queries, near_sum, maxima,
    q_send, q_recv, kv_send, kv_recv, rope_send, rope_recv, seg_send, seg_recv, w_send, w_recv, max_send, max_recv, local,
):
    s = lax.axis_index("seq")
    h = lax.axis_index("head")
    rows = q_lat.shape[0]
    part = rope.shape[0] // m
    pairs = own // 2
    q_rows = w_nope.shape[0]
    kv_rows = w_kv.shape[0]
    half = n // 2
    routes = [("seq", stride) for stride in halvings(n)] + [("head", stride) for stride in halvings(m)]
    last = len([1 for axis, _ in routes if axis == "seq"])

    barrier = pltpu.get_barrier_semaphore()
    for k in range(1, n):
        pl.semaphore_signal(barrier, inc=1, device_id=(flip(s, k), h), device_id_type=MESH)
    for stride in halvings(m):
        pl.semaphore_signal(barrier, inc=1, device_id=(s, other(h, stride)), device_id_type=MESH)

    def window(whole, width, ps, ph):
        return whole.at[pl.ds(pl.multiple_of(ps * rows, rows), rows), pl.ds(pl.multiple_of(ph * width, LANES), width)]

    def places(k, g):
        ps, ph = flip(s, k), flip(h, g)
        return (
            window(q_all, q_lat.shape[1], ps, ph),
            window(kv_all, kv_lat.shape[1], ps, ph),
            rope_all.at[ps, pl.ds(pl.multiple_of(ph * part, part), part), :],
        )

    def parts_of(p):
        found = []
        for j in range(pairs):
            even = pl.ds(pl.multiple_of((p * own + 2 * j) * LANES, LANES), LANES)
            odd = pl.ds(pl.multiple_of((p * own + 2 * j + 1) * LANES, LANES), LANES)
            both = pl.ds(pl.multiple_of((p * pairs + j) * LANES, LANES), LANES)
            found.append((w_nope.at[:, even], w_even, j, slice(0, LANES)))
            found.append((w_rope.at[:, both], w_even, j, slice(LANES, 2 * LANES)))
            found.append((w_nope.at[:, odd], w_odd, j, slice(0, LANES)))
        found.append((w_kv.at[:, pl.ds(pl.multiple_of(p * own * LANES, LANES), own * LANES)], w_key, None, None))
        return found

    def landing(target, j, columns, source):
        if j is None:
            return target.at[pl.ds(pl.multiple_of(source * kv_rows, kv_rows), kv_rows), :]
        return target.at[j, pl.ds(pl.multiple_of(source * q_rows, q_rows), q_rows), columns]

    own_pieces = (q_lat, kv_lat, rope.at[pl.ds(pl.multiple_of(h * part, part), part), :], segs)
    loads = [
        pltpu.make_async_copy(src, dst, local.at[i])
        for i, (src, dst) in enumerate(zip(own_pieces, places(0, 0) + (segs_all.at[s],)))
    ]
    for copy in loads:
        copy.start()
    keeps = [
        pltpu.make_async_copy(src, landing(target, j, columns, s), local.at[4 + i])
        for i, (src, target, j, columns) in enumerate(parts_of(s))
    ] + [
        pltpu.make_async_copy(src, dst, local.at[4 + len(parts_of(s)) + i])
        for i, (src, dst) in enumerate(zip((w_nope, w_rope, w_kv), (held_nope, held_rope, held_kv)))
    ]
    for copy in keeps:
        copy.start()
    pl.semaphore_wait(barrier, n - 1 + len(halvings(m)))
    for copy in loads:
        copy.wait()

    drains = []
    slots = [0]

    def push(k, g, route):
        axis, stride = route
        target = (other(s, stride), h) if axis == "seq" else (s, other(h, stride))
        at = (k ^ stride) * m + g if axis == "seq" else k * m + (g ^ stride)
        slot = slots[0]
        slots[0] += 1
        for ref, sent, taken in zip(places(k, g), (q_send, kv_send, rope_send), (q_recv, kv_recv, rope_recv)):
            copy = pltpu.make_async_remote_copy(
                src_ref=ref, dst_ref=ref, send_sem=sent.at[slot], recv_sem=taken.at[at],
                device_id=target, device_id_type=MESH)
            copy.start()
            drains.append((ref, sent.at[slot]))

    def relay(k, g):
        for ref, taken in zip(places(k, g), (q_recv, kv_recv, rope_recv)):
            pltpu.make_async_copy(ref, ref, taken.at[k * m + g]).wait()
        reached = max(i for i, (axis, stride) in enumerate(routes) if (k if axis == "seq" else g) & stride)
        for route in routes[reached + 1:]:
            push(k, g, route)

    def weights(wanted, k):
        p = flip(s, k)
        for i, (src, target, j, columns) in enumerate(parts_of(p)):
            if i in wanted:
                copy = pltpu.make_async_remote_copy(
                    src_ref=src, dst_ref=landing(target, j, columns, s),
                    send_sem=w_send.at[i * n + k], recv_sem=w_recv.at[i * n + k],
                    device_id=(p, h), device_id_type=MESH)
                copy.start()
                drains.append((src, w_send.at[i * n + k]))

    def take(j, wanted, ks):
        for k in ks:
            for i in wanted:
                target, columns = ((w_even, slice(0, LANES)), (w_even, slice(LANES, 2 * LANES)), (w_odd, slice(0, LANES)))[i]
                ref = landing(target, j, columns, flip(s, k))
                pltpu.make_async_copy(ref, ref, w_recv.at[(3 * j + i) * n + k]).wait()

    far = [k ^ half for k in range(half)]
    near = list(range(half - 1, 0, -1))
    kv_part = 3 * pairs
    first = [0, 1]
    later = [[kv_part]] + [[2]] + [group for j in range(1, pairs) for group in ([3 * j, 3 * j + 1], [3 * j + 2])]

    for route in routes:
        push(0, 0, route)
    for k in range(1, n):
        copy = pltpu.make_async_remote_copy(
            src_ref=segs_all.at[s], dst_ref=segs_all.at[s], send_sem=seg_send.at[k], recv_sem=seg_recv.at[k],
            device_id=(flip(s, k), h), device_id_type=MESH)
        copy.start()
        drains.append((segs_all.at[s], seg_send.at[k]))
    for k in far:
        weights(first, k)
    order = sorted(range(1, n), key=lambda k: (bin(k).count("1"), k & 1 == 1 and bin(k).count("1") > 1, k))
    on_links = max(i for i, k in enumerate(order) if k & 1 == 0)
    for k in order[: on_links + 1]:
        relay(k, 0)
    for k in near:
        weights(first, k)
    for wanted in later:
        for k in far + near:
            weights(wanted, k)

    for k in range(1, n):
        ref = segs_all.at[flip(s, k)]
        pltpu.make_async_copy(ref, ref, seg_recv.at[k]).wait()

    def fill_segs(block, carry):
        here = pl.ds(pl.multiple_of(block * rows, rows), rows)
        seg_cols[here, :] = jnp.transpose(jnp.broadcast_to(segs_all[block], (LANES, rows)))
        return carry

    lax.fori_loop(0, n, fill_segs, 0)
    reach = (REACH + 1) * rows

    def range_of(block):
        start = jnp.maximum(block - REACH, 0) * rows
        return start, pl.ds(pl.multiple_of(start, rows), reach)

    def fill_caps(block, carry):
        start, span = range_of(block)
        key_segs = jnp.concatenate([seg_cols[span, :]] * (rows // LANES), 1)
        key_pos = start + lax.broadcasted_iota(jnp.int32, (reach, rows), 0)
        query_pos = block * rows + lax.broadcasted_iota(jnp.int32, (reach, rows), 1)
        allowed = (key_segs == segs_all[block]) & (key_pos <= query_pos)
        caps[block] = jnp.where(allowed, jnp.float32(3.4e38), jnp.float32(-1e30))
        return carry

    lax.fori_loop(0, n, fill_caps, 0)

    for k in order[on_links + 1:]:
        relay(k, 0)
    for g in range(1, m):
        for k in [0] + order:
            relay(k, g)

    for copy in keeps:
        copy.wait()
    for k in far + near:
        ref = landing(w_key, None, None, flip(s, k))
        pltpu.make_async_copy(ref, ref, w_recv.at[kv_part * n + k]).wait()
    q_scale = 1.0 / math.sqrt(QLORA)
    k_scale = 1.0 / math.sqrt(KVLORA)
    lane = lax.broadcasted_iota(jnp.int32, (rows, LANES), 1)
    sides = LANES // D_ROPE

    def fill_keys(block, carry):
        here = pl.ds(pl.multiple_of(block * rows, rows), rows)
        key = (jnp.dot(kv_all[here, :], w_key[...], preferred_element_type=jnp.float32) * k_scale).astype(jnp.bfloat16)
        turned = jnp.concatenate([rope_all[block].astype(jnp.float32)] * sides, 0)
        twice = jnp.transpose(turned).astype(jnp.bfloat16)
        for i in range(own):
            side = jnp.where(lane // D_ROPE == i % sides, twice, jnp.zeros_like(twice))
            keys[i, here, :] = jnp.concatenate([key[:, i * D_NOPE : (i + 1) * D_NOPE], side], 1)
        return carry

    lax.fori_loop(0, n, fill_keys, 0)

    def top_logits(i, block, q_head):
        first = max(block - REACH, 0)
        best = None
        for other_block in range(first, block + 1):
            logits = lax.dot_general(
                keys[i, other_block * rows : (other_block + 1) * rows, :], q_head,
                (((1,), (1,)), ((), ())), preferred_element_type=jnp.float32,
            )
            cap = caps[block, (other_block - first) * rows : (other_block - first + 1) * rows, :]
            top = jnp.max(jnp.minimum(logits, cap).reshape(rows // 8, 8, rows), axis=0)
            best = top if best is None else jnp.maximum(best, top)
        top = jnp.max(best, axis=0, keepdims=True) * (1.0 / math.sqrt(D_NOPE + D_ROPE))
        maxima[pl.ds(i, 1), block * rows : (block + 1) * rows] = top

    depth = half * q_rows
    close = pl.multiple_of(s // half * depth, depth)
    distant = pl.multiple_of((1 - s // half) * depth, depth)

    def head_pair(j, carry):
        take(j, (0, 1), far + near)
        for block in range(n):
            here = slice(block * rows, (block + 1) * rows)
            query = jnp.dot(q_all[here, :], w_even[j], preferred_element_type=jnp.float32)
            queries[here, :] = (query * q_scale).astype(jnp.bfloat16)
        for block in range(n):
            top_logits(2 * j, block, queries[block * rows : (block + 1) * rows, :])
        take(j, (2,), near)
        for block in range(n):
            here = slice(block * rows, (block + 1) * rows)
            near_sum[here, :] = jnp.dot(
                q_all[here, pl.ds(close, depth)], w_odd[j, pl.ds(close, depth), :], preferred_element_type=jnp.float32
            )
        take(j, (2,), far)
        for block in range(n):
            here = slice(block * rows, (block + 1) * rows)
            query = near_sum[here, :] + jnp.dot(
                q_all[here, pl.ds(distant, depth)], w_odd[j, pl.ds(distant, depth), :], preferred_element_type=jnp.float32
            )
            queries[here, 0:LANES] = (query * q_scale).astype(jnp.bfloat16)
        for block in range(n):
            top_logits(2 * j + 1, block, queries[block * rows : (block + 1) * rows, :])
        return carry

    lax.fori_loop(0, pairs, head_pair, 0)

    best = jnp.max(maxima[0:own, :], axis=1, keepdims=True)
    maxima[own : 2 * own, :] = jnp.broadcast_to(best, (own, maxima.shape[1]))
    shares = []
    for k in range(1, n):
        p = flip(s, k)
        copy = pltpu.make_async_remote_copy(
            src_ref=maxima.at[:, pl.ds(pl.multiple_of(p * rows, rows), rows)], dst_ref=got.at[s],
            send_sem=max_send.at[k], recv_sem=max_recv.at[k], device_id=(p, h), device_id_type=MESH)
        copy.start()
        shares.append(copy)
    got[s] = maxima[:, pl.ds(pl.multiple_of(s * rows, rows), rows)]
    for ref, sent in drains:
        pltpu.make_async_copy(ref, ref, sent).wait()
    for k, copy in zip(range(1, n), shares):
        copy.wait_send()
        at = got.at[flip(s, k)]
        pltpu.make_async_copy(at, at, max_recv.at[k]).wait()


def layer(n, m, own, q_lat, kv_lat, rope, segs, w_nope, w_rope, w_kv):
    rows = q_lat.shape[0]
    tokens = n * rows
    pairs = own // 2
    moves = n * m - 1
    parts = 3 * pairs + 1
    any_ref = pl.BlockSpec(memory_space=pl.ANY)
    dma = pltpu.SemaphoreType.DMA
    kind = q_lat.dtype
    return pl.pallas_call(
        functools.partial(layer_kernel, n, m, own),
        out_shape=(pltpu.VMEM((n, 2 * own, rows), jnp.float32),)
        + tuple(pltpu.VMEM(w.shape, w.dtype) for w in (w_nope, w_rope, w_kv)),
        in_specs=[any_ref] * 7,
        out_specs=(pl.BlockSpec(memory_space=pltpu.VMEM),) * 4,
        scratch_shapes=[
            pltpu.VMEM((tokens, m * q_lat.shape[1]), kind),
            pltpu.VMEM((tokens, m * kv_lat.shape[1]), kind),
            pltpu.VMEM((n,) + rope.shape, kind),
            pltpu.VMEM((n,) + segs.shape, jnp.int32),
            pltpu.VMEM((pairs, n * w_nope.shape[0], 2 * LANES), kind),
            pltpu.VMEM((pairs, n * w_nope.shape[0], LANES), kind),
            pltpu.VMEM((n * w_kv.shape[0], own * LANES), kind),
            pltpu.VMEM((own, tokens, D_NOPE + LANES), kind),
            pltpu.VMEM((n, (REACH + 1) * rows, rows), jnp.float32),
            pltpu.VMEM((tokens, LANES), jnp.int32),
            pltpu.VMEM((tokens, 2 * LANES), kind),
            pltpu.VMEM((tokens, LANES), jnp.float32),
            pltpu.VMEM((2 * own, tokens), jnp.float32),
            dma((moves,)), dma((n * m,)), dma((moves,)), dma((n * m,)), dma((moves,)), dma((n * m,)),
            dma((n,)), dma((n,)),
            dma((parts * n,)), dma((parts * n,)), dma((n,)), dma((n,)), dma((7 + parts,)),
        ],
        compiler_params=pltpu.CompilerParams(
            collective_id=0, has_side_effects=True, vmem_limit_bytes=60 * 1024 * 1024
        ),
        name="layer",
    )(*(pltpu.with_memory_space_constraint(a, pltpu.HBM) for a in (q_lat, kv_lat, rope, segs, w_nope, w_rope, w_kv)))


def clip_kernel(
    n, own, got, threshold, w_nope, w_rope, w_kv, new_nope, new_rope, new_kv, head_max, row_max,
    out_nope, out_rope, out_kv, sems,
):
    limit = threshold[0]
    lane = lax.broadcasted_iota(jnp.int32, (1, LANES), 1)
    tops = jnp.zeros((1, head_max.shape[1]), jnp.float32)
    place = lax.broadcasted_iota(jnp.int32, tops.shape, 1)
    copies = []

    def scaled(source, target, column, factor):
        columns = slice(column * LANES, (column + 1) * LANES)
        target[:, columns] = (source[:, columns].astype(jnp.float32) * factor).astype(target.dtype)

    for s in range(n):
        top = got[s, own : 2 * own, 0:LANES]
        clip = limit / jnp.maximum(top, limit)
        root = jnp.sqrt(clip)
        for i in range(own):
            head = s * own + i
            scaled(w_nope, out_nope, head, root[i : i + 1])
            scaled(w_kv, out_kv, head, root[i : i + 1])
            tops = jnp.where(place == head, top[i : i + 1, 0 : tops.shape[1]], tops)
        for j in range(own // 2):
            factor = jnp.where(lane < D_ROPE, clip[2 * j : 2 * j + 1], clip[2 * j + 1 : 2 * j + 2])
            scaled(w_rope, out_rope, s * own // 2 + j, factor)
        for i, (source, target) in enumerate(((out_nope, new_nope), (out_rope, new_rope), (out_kv, new_kv))):
            width = source.shape[1] // n
            at = pl.ds(s * width, width)
            copy = pltpu.make_async_copy(source.at[:, at], target.at[:, at], sems.at[3 * s + i])
            copy.start()
            copies.append(copy)
        row_max[s * own : (s + 1) * own, :] = got[s, 0:own, :]
    head_max[...] = tops
    for copy in copies:
        copy.wait()


def clip_weights(n, own, got, threshold, w_nope, w_rope, w_kv):
    weights = (w_nope, w_rope, w_kv)
    heads = n * own
    in_vmem = pl.BlockSpec(memory_space=pltpu.VMEM)
    any_ref = pl.BlockSpec(memory_space=pl.ANY)
    return pl.pallas_call(
        functools.partial(clip_kernel, n, own),
        out_shape=tuple(jax.ShapeDtypeStruct(w.shape, w.dtype) for w in weights)
        + (jax.ShapeDtypeStruct((1, heads), jnp.float32), jax.ShapeDtypeStruct((heads, got.shape[2]), jnp.float32)),
        in_specs=[in_vmem, pl.BlockSpec(memory_space=pltpu.SMEM)] + [in_vmem] * 3,
        out_specs=(any_ref,) * 3 + (in_vmem,) * 2,
        scratch_shapes=[pltpu.VMEM(w.shape, w.dtype) for w in weights] + [pltpu.SemaphoreType.DMA((3 * n,))],
        compiler_params=pltpu.CompilerParams(vmem_limit_bytes=16 * 1024 * 1024),
        name="clip_weights",
    )(
        pltpu.with_memory_space_constraint(got, pltpu.VMEM),
        threshold,
        *(pltpu.with_memory_space_constraint(w, pltpu.VMEM) for w in weights),
    )


def owned_body(n, m, q_latent, kv_latent, k_rope, segment_ids, w_q_nope, w_q_rope, w_kv_nope, threshold):
    rows = q_latent.shape[0]
    heads = w_q_nope.shape[1] // D_NOPE
    own = heads // n
    got, *held = layer(
        n, m, own, q_latent, kv_latent, k_rope.T, segment_ids.reshape(1, rows), w_q_nope, w_q_rope, w_kv_nope
    )
    new_nope, new_rope, new_kv, head_max, row_max = clip_weights(n, own, got, threshold, *held)
    return (new_nope, new_rope, new_kv, head_max.reshape(heads), row_max.T)


def body(n, m, *operands):
    heads = operands[4].shape[1] // D_NOPE
    rows = operands[0].shape[0]
    shares = heads % n == 0 and heads // n % 4 == 0 and heads <= LANES
    powers = n & (n - 1) == 0 and m & (m - 1) == 0 and n > REACH
    small = n * rows * operands[0].shape[1] * m <= 2048 * 1536
    if shares and powers and small and rows % LANES == 0 and operands[2].shape[1] % (16 * m) == 0:
        return owned_body(n, m, *operands)
    return grouped_body(*operands)


def solution(mesh):
    in_specs = (
        P("seq", "head"),
        P("seq", "head"),
        P("seq", None),
        P("seq"),
        P("seq", "head"),
        P("seq", "head"),
        P("seq", "head"),
        P(),
    )
    out_specs = (P("seq", "head"), P("seq", "head"), P("seq", "head"), P("head"), P("seq", "head"))
    return jax.shard_map(functools.partial(body, mesh.shape["seq"], mesh.shape["head"]), mesh=mesh, in_specs=in_specs, out_specs=out_specs, check_vma=False)
```

```python
import functools
import math

import jax
import jax.numpy as jnp
from jax import lax
from jax.experimental import pallas as pl
from jax.experimental.pallas import tpu as pltpu
from jax.sharding import PartitionSpec as P

D_NOPE = 128
D_ROPE = 64
QLORA = 1536
KVLORA = 512
REACH = 3


def as_sent(value):
    return jax.tree.map(lambda a: a.astype(jnp.bfloat16) if a.dtype == jnp.float32 else a, value)


def from_partner(value, axis, stride):
    mask = 2**stride
    pairs = [(source, source ^ mask) for source in range(lax.axis_size(axis))]
    return lax.ppermute(value, axis, pairs)


def shifted(block, axis, distance):
    devices = range(lax.axis_size(axis))
    route = [(i - distance, i) for i in devices if i - distance in devices]
    return lax.ppermute(block, axis, route)


def score_max(query_nope, query_rope, key_nope, key_rope, allowed):
    nope = jnp.einsum("qhd,khd->hqk", query_nope, key_nope, preferred_element_type=jnp.float32)
    rope = jnp.einsum("qhd,kd->hqk", query_rope, key_rope, preferred_element_type=jnp.float32)
    scores = (nope + rope) * (1.0 / math.sqrt(D_NOPE + D_ROPE))
    return jnp.max(jnp.where(allowed[None], scores, jnp.float32(-1e30)), axis=2)


def masked_max(compute, operands):
    return compute(*operands)


def spread_columns(weight, width, quarter, copies):
    pieces = weight.reshape(weight.shape[0], 4, quarter * width).transpose(1, 0, 2)
    return jnp.tile(pieces, (copies, 1, 1))


def grouped_body(q_latent, kv_latent, k_rope, segment_ids, w_q_nope, w_q_rope, w_kv_nope, threshold):
    q_whole, kv_whole = (
        lax.all_gather(q_latent, "head", axis=1, tiled=True),
        lax.all_gather(kv_latent, "head", axis=1, tiled=True),
    )
    rows = q_whole.shape[0]
    heads = w_q_nope.shape[1] // D_NOPE
    q_scale = 1.0 / math.sqrt(QLORA)
    k_scale = 1.0 / math.sqrt(KVLORA)
    place = lax.axis_index("seq")
    quarter = heads // 4
    copies = lax.axis_size("seq") // 4
    slot = place % 4
    sent = (
        spread_columns(w_q_nope, D_NOPE, quarter, copies),
        spread_columns(w_q_rope, D_ROPE, quarter, copies),
        spread_columns(w_kv_nope, D_NOPE, quarter, copies),
    )
    got_nope, got_rope, got_kv = (
        lax.all_to_all(sent[0], "seq", split_axis=0, concat_axis=1, tiled=True),
        lax.all_to_all(sent[1], "seq", split_axis=0, concat_axis=1, tiled=True),
        lax.all_to_all(sent[2], "seq", split_axis=0, concat_axis=1, tiled=True),
    )
    sub_nope = got_nope.reshape(QLORA, quarter * D_NOPE)
    sub_rope = got_rope.reshape(QLORA, quarter * D_ROPE)
    sub_kv = got_kv.reshape(KVLORA, quarter * D_NOPE)
    group = (q_whole, kv_whole, k_rope)
    for level in range(2):
        partner = jax.tree.map(
            lambda part, own: part.astype(own.dtype),
            from_partner(as_sent(group), "seq", level),
            group,
        )
        upper = place // (1 << level) % 2 == 1
        group = tuple(
            (
                jnp.where(
                    upper, jnp.concatenate([other, mine], 0), jnp.concatenate([mine, other], 0)
                )
                for mine, other in zip(group, partner)
            )
        )
    group_q, group_kv, group_rope = group
    early_kv, early_rope = shifted(
        (group_kv[(4 - REACH) * rows :], group_rope[(4 - REACH) * rows :]), "seq", 4
    )
    keys_kv = jnp.concatenate([early_kv, group_kv], 0)
    keys_rope = jnp.concatenate([early_rope, group_rope], 0)
    key_nope = (
        (jnp.dot(keys_kv, sub_kv, preferred_element_type=jnp.float32) * k_scale)
        .astype(jnp.bfloat16)
        .reshape(keys_kv.shape[0], quarter, D_NOPE)
    )
    query_nope = (
        (jnp.dot(group_q, sub_nope, preferred_element_type=jnp.float32) * q_scale)
        .astype(jnp.bfloat16)
        .reshape(4 * rows, quarter, D_NOPE)
    )
    query_rope = (
        (jnp.dot(group_q, sub_rope, preferred_element_type=jnp.float32) * q_scale)
        .astype(jnp.bfloat16)
        .reshape(4 * rows, quarter, D_ROPE)
    )
    all_segs = lax.all_gather(segment_ids, "seq", axis=0, tiled=True)
    padded_segs = jnp.concatenate([jnp.full((REACH * rows,), -1, jnp.int32), all_segs], 0)
    first = place // 4 * 4
    window = (REACH + 1) * rows
    block_rows = []
    for local in range(4):
        block = first + local
        query_seg = lax.dynamic_slice_in_dim(all_segs, block * rows, rows, 0)
        key_seg = lax.dynamic_slice_in_dim(padded_segs, block * rows, window, 0)
        query_pos = block * rows + jnp.arange(rows, dtype=jnp.int32)
        key_pos = (block - REACH) * rows + jnp.arange(window, dtype=jnp.int32)
        allowed = (
            (query_seg[:, None] == key_seg[None, :])
            & (key_pos[None, :] <= query_pos[:, None])
            & (key_pos[None, :] >= 0)
        )
        operands = (
            query_nope[local * rows : (local + 1) * rows],
            query_rope[local * rows : (local + 1) * rows],
            key_nope[local * rows : local * rows + window],
            keys_rope[local * rows : local * rows + window],
            allowed,
        )
        block_rows.append(masked_max(score_max, operands))
    stacked = jnp.stack(block_rows, 0)[None]
    for level in range(2):
        partner = from_partner(stacked, "seq", level)
        upper = place // (1 << level) % 2 == 1
        stacked = jnp.where(
            upper, jnp.concatenate([partner, stacked], 0), jnp.concatenate([stacked, partner], 0)
        )
    own = lax.dynamic_index_in_dim(stacked, slot, 1, False)
    row_max = own.reshape(heads, rows).T
    local_heads = jnp.max(row_max, axis=0)
    head_max = lax.pmax(local_heads, "seq")
    return finish(threshold, head_max, row_max, w_q_nope, w_q_rope, w_kv_nope)


def finish(threshold, head_max, row_max, w_q_nope, w_q_rope, w_kv_nope):
    clip = threshold[0] / jnp.maximum(head_max, threshold[0])
    root = jnp.sqrt(clip)
    new_q_nope = (w_q_nope.astype(jnp.float32) * jnp.repeat(root, D_NOPE)[None, :]).astype(
        jnp.bfloat16
    )
    new_q_rope = (w_q_rope.astype(jnp.float32) * jnp.repeat(clip, D_ROPE)[None, :]).astype(
        jnp.bfloat16
    )
    new_kv_nope = (w_kv_nope.astype(jnp.float32) * jnp.repeat(root, D_NOPE)[None, :]).astype(
        jnp.bfloat16
    )
    return (new_q_nope, new_q_rope, new_kv_nope, head_max, row_max)


MESH = pl.DeviceIdType.MESH
LANES = 128
EVEN_NOPE, PAIR_ROPE, ODD_NOPE, EVEN_KEY, ODD_KEY = KINDS = range(5)


def other(index, stride):
    return index + stride - 2 * stride * (index // stride % 2)


def flip(index, bits):
    stride = 1
    while stride <= bits:
        if bits & stride:
            index = other(index, stride)
        stride *= 2
    return index


def halvings(size):
    return [size >> (i + 1) for i in range(size.bit_length() - 1)]


def layer_kernel(
    n, m, own, q_lat, kv_lat, rope, segs, threshold, w_nope, w_rope, w_kv,
    got_early, got_late, held_nope, held_rope, held_kv,
    q_all, kv_all, rope_all, segs_all, w_even, w_odd, w_key, keys, caps, seg_cols, queries, near_sum, maxima, early, late,
    q_send, q_recv, kv_send, kv_recv, rope_send, rope_recv, seg_send, seg_recv, w_send, w_recv, early_send, early_recv, late_send, late_recv, local,
):
    s = lax.axis_index("seq")
    h = lax.axis_index("head")
    rows = q_lat.shape[0]
    part = rope.shape[0] // m
    pairs = own // 2
    q_rows = w_nope.shape[0]
    kv_rows = w_kv.shape[0]
    half = n // 2
    routes = [("seq", stride) for stride in halvings(n)] + [("head", stride) for stride in halvings(m)]
    last = len([1 for axis, _ in routes if axis == "seq"])

    barrier = pltpu.get_barrier_semaphore()
    for k in range(1, n):
        pl.semaphore_signal(barrier, inc=1, device_id=(flip(s, k), h), device_id_type=MESH)
    for stride in halvings(m):
        pl.semaphore_signal(barrier, inc=1, device_id=(s, other(h, stride)), device_id_type=MESH)

    def window(whole, width, ps, ph):
        return whole.at[pl.ds(pl.multiple_of(ps * rows, rows), rows), pl.ds(pl.multiple_of(ph * width, LANES), width)]

    def places(k, g):
        ps, ph = flip(s, k), flip(h, g)
        return (
            window(q_all, q_lat.shape[1], ps, ph),
            window(kv_all, kv_lat.shape[1], ps, ph),
            rope_all.at[ps, pl.ds(pl.multiple_of(ph * part, part), part), :],
        )

    def lanes(index, count=1):
        return pl.ds(pl.multiple_of(index * LANES, LANES), count * LANES)

    def parts_of(p):
        found = []
        for j in range(pairs):
            found.append(w_nope.at[:, lanes(p * own + 2 * j)])
            found.append(w_rope.at[:, lanes(p * pairs + j)])
            found.append(w_nope.at[:, lanes(p * own + 2 * j + 1)])
            found.append(w_kv.at[:, lanes(p * own + 2 * j)])
            found.append(w_kv.at[:, lanes(p * own + 2 * j + 1)])
        return found

    def landing(j, kind, source):
        q_at = pl.ds(pl.multiple_of(source * q_rows, q_rows), q_rows)
        kv_at = pl.ds(pl.multiple_of(source * kv_rows, kv_rows), kv_rows)
        if kind < EVEN_KEY:
            return (w_even.at[j, q_at, 0:LANES], w_even.at[j, q_at, LANES : 2 * LANES], w_odd.at[j, q_at, :])[kind]
        return w_key.at[2 * j + kind - EVEN_KEY, kv_at, :]

    own_pieces = (q_lat, kv_lat, rope.at[pl.ds(pl.multiple_of(h * part, part), part), :], segs)
    loads = [
        pltpu.make_async_copy(src, dst, local.at[i])
        for i, (src, dst) in enumerate(zip(own_pieces, places(0, 0) + (segs_all.at[s],)))
    ]
    for copy in loads:
        copy.start()
    keeps = [
        pltpu.make_async_copy(src, landing(i // len(KINDS), i % len(KINDS), s), local.at[4 + i])
        for i, src in enumerate(parts_of(s))
    ] + [
        pltpu.make_async_copy(src, dst, local.at[4 + len(parts_of(s)) + i])
        for i, (src, dst) in enumerate(zip((w_nope, w_rope, w_kv), (held_nope, held_rope, held_kv)))
    ]
    for copy in keeps:
        copy.start()
    pl.semaphore_wait(barrier, n - 1 + len(halvings(m)))
    for copy in loads:
        copy.wait()

    drains = []
    slots = [0]

    def push(k, g, route):
        axis, stride = route
        target = (other(s, stride), h) if axis == "seq" else (s, other(h, stride))
        at = (k ^ stride) * m + g if axis == "seq" else k * m + (g ^ stride)
        slot = slots[0]
        slots[0] += 1
        for ref, sent, taken in zip(places(k, g), (q_send, kv_send, rope_send), (q_recv, kv_recv, rope_recv)):
            copy = pltpu.make_async_remote_copy(
                src_ref=ref, dst_ref=ref, send_sem=sent.at[slot], recv_sem=taken.at[at],
                device_id=target, device_id_type=MESH)
            copy.start()
            drains.append((ref, sent.at[slot]))

    def relay(k, g):
        for ref, taken in zip(places(k, g), (q_recv, kv_recv, rope_recv)):
            pltpu.make_async_copy(ref, ref, taken.at[k * m + g]).wait()
        reached = max(i for i, (axis, stride) in enumerate(routes) if (k if axis == "seq" else g) & stride)
        for route in routes[reached + 1:]:
            push(k, g, route)

    def weights(j, wanted, k):
        p = flip(s, k)
        sources = parts_of(p)
        for kind in wanted:
            i = j * len(KINDS) + kind
            copy = pltpu.make_async_remote_copy(
                src_ref=sources[i], dst_ref=landing(j, kind, s),
                send_sem=w_send.at[i * n + k], recv_sem=w_recv.at[i * n + k],
                device_id=(p, h), device_id_type=MESH)
            copy.start()
            drains.append((sources[i], w_send.at[i * n + k]))

    def take(j, wanted, ks):
        for k in ks:
            for kind in wanted:
                ref = landing(j, kind, flip(s, k))
                pltpu.make_async_copy(ref, ref, w_recv.at[(j * len(KINDS) + kind) * n + k]).wait()

    far = [k ^ half for k in range(half)]
    near = list(range(half - 1, 0, -1))
    first = (EVEN_NOPE, PAIR_ROPE)
    later = [(0, (EVEN_KEY,)), (0, (ODD_NOPE,)), (0, (ODD_KEY,))]
    for j in range(1, pairs):
        later += [(j, first + (EVEN_KEY,)), (j, (ODD_NOPE,)), (j, (ODD_KEY,))]

    for route in routes:
        push(0, 0, route)
    for k in range(1, n):
        copy = pltpu.make_async_remote_copy(
            src_ref=segs_all.at[s], dst_ref=segs_all.at[s], send_sem=seg_send.at[k], recv_sem=seg_recv.at[k],
            device_id=(flip(s, k), h), device_id_type=MESH)
        copy.start()
        drains.append((segs_all.at[s], seg_send.at[k]))
    for k in far:
        weights(0, first, k)
    order = sorted(range(1, n), key=lambda k: (bin(k).count("1"), k & 1 == 1 and bin(k).count("1") > 1, k))
    on_links = max(i for i, k in enumerate(order) if k & 1 == 0)
    for k in order[: on_links + 1]:
        relay(k, 0)
    for k in near:
        weights(0, first, k)
    for j, wanted in later:
        for k in far + near:
            weights(j, wanted, k)

    for k in range(1, n):
        ref = segs_all.at[flip(s, k)]
        pltpu.make_async_copy(ref, ref, seg_recv.at[k]).wait()

    def fill_segs(block, carry):
        here = pl.ds(pl.multiple_of(block * rows, rows), rows)
        seg_cols[here, :] = jnp.transpose(jnp.broadcast_to(segs_all[block], (LANES, rows)))
        return carry

    lax.fori_loop(0, n, fill_segs, 0)
    reach = (REACH + 1) * rows

    def range_of(block):
        start = jnp.maximum(block - REACH, 0) * rows
        return start, pl.ds(pl.multiple_of(start, rows), reach)

    def fill_caps(block, carry):
        start, span = range_of(block)
        key_segs = jnp.concatenate([seg_cols[span, :]] * (rows // LANES), 1)
        key_pos = start + lax.broadcasted_iota(jnp.int32, (reach, rows), 0)
        query_pos = block * rows + lax.broadcasted_iota(jnp.int32, (reach, rows), 1)
        allowed = (key_segs == segs_all[block]) & (key_pos <= query_pos)
        caps[block] = jnp.where(allowed, jnp.float32(3.4e38), jnp.float32(-1e30))
        return carry

    lax.fori_loop(0, n, fill_caps, 0)

    for k in order[on_links + 1:]:
        relay(k, 0)
    for g in range(1, m):
        for k in [0] + order:
            relay(k, g)

    for copy in keeps:
        copy.wait()
    q_scale = 1.0 / math.sqrt(QLORA)
    k_scale = 1.0 / math.sqrt(KVLORA)
    lane = lax.broadcasted_iota(jnp.int32, (rows, LANES), 1)
    sides = LANES // D_ROPE
    spare = rows // LANES

    def fill_sides(block, carry):
        here = pl.ds(pl.multiple_of(block * rows, rows), rows)
        turned = jnp.concatenate([rope_all[block].astype(jnp.float32)] * sides, 0)
        twice = jnp.transpose(turned).astype(jnp.bfloat16)
        for i in range(own):
            keys[i, here, LANES : 2 * LANES] = jnp.where(lane // D_ROPE == i % sides, twice, jnp.zeros_like(twice))
        return carry

    lax.fori_loop(0, n, fill_sides, 0)
    maxima[...] = jnp.zeros_like(maxima)

    def span(block):
        return slice(block * rows, (block + 1) * rows)

    def top_logits(i, block):
        first = max(block - REACH, 0)
        best = None
        for other_block in range(first, block + 1):
            logits = lax.dot_general(
                keys[i, span(other_block), :], queries[span(block), :],
                (((1,), (1,)), ((), ())), preferred_element_type=jnp.float32,
            )
            cap = caps[block, span(other_block - first), :]
            top = jnp.max(jnp.minimum(logits, cap).reshape(rows // 8, 8, rows), axis=0)
            best = top if best is None else jnp.maximum(best, top)
        top = jnp.max(best, axis=0, keepdims=True) * (1.0 / math.sqrt(D_NOPE + D_ROPE))
        maxima[pl.ds(i, 1), span(block)] = top
        return top

    depth = half * kv_rows
    close = pl.multiple_of(s // half * depth, depth)
    distant = pl.multiple_of((1 - s // half) * depth, depth)

    def share_early():
        early[0:own, :] = maxima[...]
        early[own : 2 * own, :] = jnp.broadcast_to(jnp.max(maxima[...], axis=1, keepdims=True), maxima.shape)
        for k in range(1, n):
            p = flip(s, k)
            pltpu.make_async_remote_copy(
                src_ref=early.at[:, pl.ds(pl.multiple_of(p * rows, rows), rows)], dst_ref=got_early.at[s],
                send_sem=early_send.at[k], recv_sem=early_recv.at[k], device_id=(p, h), device_id_type=MESH).start()
        got_early[s] = early[:, pl.ds(pl.multiple_of(s * rows, rows), rows)]

    def scale_early():
        for k in range(1, n):
            gone = early.at[:, pl.ds(pl.multiple_of(flip(s, k) * rows, rows), rows)]
            pltpu.make_async_copy(gone, gone, early_send.at[k]).wait()
            come = got_early.at[flip(s, k)]
            pltpu.make_async_copy(come, come, early_recv.at[k]).wait()
        for p in range(n):
            clip = clip_of(got_early[p, own : 2 * own, 0:LANES], threshold[0])
            root = jnp.sqrt(clip)
            for i in range(own - 1):
                at = slice((p * own + i) * LANES, (p * own + i + 1) * LANES)
                scale_columns(held_nope, at, held_nope, at, root[i : i + 1])
                scale_columns(held_kv, at, held_kv, at, root[i : i + 1])
            for j in range(pairs):
                at = slice((p * pairs + j) * LANES, (p * pairs + j + 1) * LANES)
                odd = clip[2 * j + 1 : 2 * j + 2] if j < pairs - 1 else jnp.ones((1, LANES), jnp.float32)
                factor = jnp.where(lane[0:1] < D_ROPE, clip[2 * j : 2 * j + 1], odd)
                scale_columns(held_rope, at, held_rope, at, factor)

    def head_pair(j, carry):
        take(j, (EVEN_KEY,), far + near)
        for block in range(n):
            key = jnp.dot(kv_all[span(block), :], w_key[2 * j], preferred_element_type=jnp.float32)
            keys[2 * j, span(block), 0:LANES] = (key * k_scale).astype(jnp.bfloat16)
        take(j, first, far + near)
        for block in range(n):
            query = jnp.dot(q_all[span(block), :], w_even[j], preferred_element_type=jnp.float32)
            queries[span(block), :] = (query * q_scale).astype(jnp.bfloat16)
        for block in range(n):
            top_logits(2 * j, block)
        pl.when(j == pairs - 1)(share_early)
        take(j, (ODD_NOPE,), far + near)
        for block in range(n):
            query = jnp.dot(q_all[span(block), :], w_odd[j], preferred_element_type=jnp.float32)
            queries[span(block), 0:LANES] = (query * q_scale).astype(jnp.bfloat16)
        take(j, (ODD_KEY,), near)
        for block in range(n):
            near_sum[span(block), :] = jnp.dot(
                kv_all[span(block), pl.ds(close, depth)], w_key[2 * j + 1, pl.ds(close, depth), :],
                preferred_element_type=jnp.float32,
            )
        pl.when(j == pairs - 1)(scale_early)
        take(j, (ODD_KEY,), far)
        for block in range(n):
            key = near_sum[span(block), :] + jnp.dot(
                kv_all[span(block), pl.ds(distant, depth)], w_key[2 * j + 1, pl.ds(distant, depth), :],
                preferred_element_type=jnp.float32,
            )
            keys[2 * j + 1, span(block), 0:LANES] = (key * k_scale).astype(jnp.bfloat16)
        best = None
        for block in range(n):
            top = top_logits(2 * j + 1, block)
            for c in range(spare):
                late[block, c : c + 1, :] = top[:, c * LANES : (c + 1) * LANES]
            best = top if best is None else jnp.maximum(best, top)
        best = jnp.broadcast_to(jnp.max(best, axis=1, keepdims=True), (late.shape[1] - spare, LANES))
        for block in range(n):
            late[block, spare : late.shape[1], :] = best
        return carry

    lax.fori_loop(0, pairs, head_pair, 0)

    for k in range(1, n):
        p = flip(s, k)
        pltpu.make_async_remote_copy(
            src_ref=late.at[p], dst_ref=got_late.at[s], send_sem=late_send.at[k], recv_sem=late_recv.at[k],
            device_id=(p, h), device_id_type=MESH).start()
        drains.append((late.at[p], late_send.at[k]))
    got_late[s] = late[s]
    for ref, sent in drains:
        pltpu.make_async_copy(ref, ref, sent).wait()
    for k in range(1, n):
        come = got_late.at[flip(s, k)]
        pltpu.make_async_copy(come, come, late_recv.at[k]).wait()


def clip_of(top, limit):
    return limit / jnp.maximum(top, limit)


def scale_columns(source, columns, target, at, factor):
    target[:, at] = (source[:, columns].astype(jnp.float32) * factor).astype(target.dtype)


def layer(n, m, own, q_lat, kv_lat, rope, segs, threshold, w_nope, w_rope, w_kv):
    rows = q_lat.shape[0]
    tokens = n * rows
    pairs = own // 2
    moves = n * m - 1
    parts = len(KINDS) * pairs
    late = rows // LANES + 2
    any_ref = pl.BlockSpec(memory_space=pl.ANY)
    dma = pltpu.SemaphoreType.DMA
    kind = q_lat.dtype
    return pl.pallas_call(
        functools.partial(layer_kernel, n, m, own),
        out_shape=(pltpu.VMEM((n, 2 * own, rows), jnp.float32), pltpu.VMEM((n, late, LANES), jnp.float32))
        + tuple(pltpu.VMEM(w.shape, w.dtype) for w in (w_nope, w_rope, w_kv)),
        in_specs=[any_ref] * 4 + [pl.BlockSpec(memory_space=pltpu.SMEM)] + [any_ref] * 3,
        out_specs=(pl.BlockSpec(memory_space=pltpu.VMEM),) * 5,
        scratch_shapes=[
            pltpu.VMEM((tokens, m * q_lat.shape[1]), kind),
            pltpu.VMEM((tokens, m * kv_lat.shape[1]), kind),
            pltpu.VMEM((n,) + rope.shape, kind),
            pltpu.VMEM((n,) + segs.shape, jnp.int32),
            pltpu.VMEM((pairs, n * w_nope.shape[0], 2 * LANES), kind),
            pltpu.VMEM((pairs, n * w_nope.shape[0], LANES), kind),
            pltpu.VMEM((own, n * w_kv.shape[0], LANES), kind),
            pltpu.VMEM((own, tokens, D_NOPE + LANES), kind),
            pltpu.VMEM((n, (REACH + 1) * rows, rows), jnp.float32),
            pltpu.VMEM((tokens, LANES), jnp.int32),
            pltpu.VMEM((tokens, 2 * LANES), kind),
            pltpu.VMEM((tokens, LANES), jnp.float32),
            pltpu.VMEM((own, tokens), jnp.float32),
            pltpu.VMEM((2 * own, tokens), jnp.float32),
            pltpu.VMEM((n, late, LANES), jnp.float32),
            dma((moves,)), dma((n * m,)), dma((moves,)), dma((n * m,)), dma((moves,)), dma((n * m,)),
            dma((n,)), dma((n,)),
            dma((parts * n,)), dma((parts * n,)), dma((n,)), dma((n,)), dma((n,)), dma((n,)), dma((7 + parts,)),
        ],
        compiler_params=pltpu.CompilerParams(
            collective_id=0, has_side_effects=True, vmem_limit_bytes=60 * 1024 * 1024
        ),
        name="layer",
    )(
        *(pltpu.with_memory_space_constraint(a, pltpu.HBM) for a in (q_lat, kv_lat, rope, segs)),
        threshold,
        *(pltpu.with_memory_space_constraint(w, pltpu.HBM) for w in (w_nope, w_rope, w_kv)),
    )


def clip_kernel(
    n, own, got_early, got_late, threshold, w_nope, w_rope, w_kv, new_nope, new_rope, new_kv, head_max, row_max,
    last_nope, last_rope, last_kv, sems,
):
    lane = lax.broadcasted_iota(jnp.int32, (1, LANES), 1)
    tops = jnp.zeros((1, head_max.shape[1]), jnp.float32)
    place = lax.broadcasted_iota(jnp.int32, tops.shape, 1)
    groups = ((w_nope, last_nope, new_nope, own), (w_rope, last_rope, new_rope, own // 2), (w_kv, last_kv, new_kv, own))
    copies = []

    def put(source, columns, target, at):
        copy = pltpu.make_async_copy(source.at[:, columns], target.at[:, at], sems.at[len(copies)])
        copy.start()
        copies.append(copy)

    for s in range(n):
        for whole, _, target, count in groups:
            ready = pl.ds(s * count * LANES, (count - 1) * LANES)
            put(whole, ready, target, ready)
    for s in range(n):
        spare = row_max.shape[1] // LANES
        clip = clip_of(got_late[s, spare : spare + 1, :], threshold[0])
        root = jnp.sqrt(clip)
        mine = slice(s * LANES, (s + 1) * LANES)
        factors = (root, jnp.where(lane < D_ROPE, 1.0, clip), root)
        for (whole, last, target, count), factor in zip(groups, factors):
            at = slice(((s + 1) * count - 1) * LANES, (s + 1) * count * LANES)
            scale_columns(whole, at, last, mine, factor)
            put(last, pl.ds(s * LANES, LANES), target, pl.ds(((s + 1) * count - 1) * LANES, LANES))
    for s in range(n):
        early = got_early[s, own : 2 * own, 0 : tops.shape[1]]
        for i in range(own - 1):
            tops = jnp.where(place == s * own + i, early[i : i + 1], tops)
        tops = jnp.where(place == s * own + own - 1, got_late[s, spare : spare + 1, 0 : tops.shape[1]], tops)
        row_max[s * own : (s + 1) * own - 1, :] = got_early[s, 0 : own - 1, :]
        for c in range(spare):
            row_max[(s + 1) * own - 1 : (s + 1) * own, c * LANES : (c + 1) * LANES] = got_late[s, c : c + 1, :]
    head_max[...] = tops
    for copy in copies:
        copy.wait()


def clip_weights(n, own, got_early, got_late, threshold, w_nope, w_rope, w_kv):
    weights = (w_nope, w_rope, w_kv)
    heads = n * own
    in_vmem = pl.BlockSpec(memory_space=pltpu.VMEM)
    any_ref = pl.BlockSpec(memory_space=pl.ANY)
    rows = got_early.shape[2]
    return pl.pallas_call(
        functools.partial(clip_kernel, n, own),
        out_shape=tuple(jax.ShapeDtypeStruct(w.shape, w.dtype) for w in weights)
        + (jax.ShapeDtypeStruct((1, heads), jnp.float32), jax.ShapeDtypeStruct((heads, rows), jnp.float32)),
        in_specs=[in_vmem] * 2 + [pl.BlockSpec(memory_space=pltpu.SMEM)] + [in_vmem] * 3,
        out_specs=(any_ref,) * 3 + (in_vmem,) * 2,
        scratch_shapes=[pltpu.VMEM((w.shape[0], n * LANES), w.dtype) for w in weights]
        + [pltpu.SemaphoreType.DMA((6 * n,))],
        compiler_params=pltpu.CompilerParams(vmem_limit_bytes=16 * 1024 * 1024),
        name="clip_weights",
    )(
        *(pltpu.with_memory_space_constraint(g, pltpu.VMEM) for g in (got_early, got_late)),
        threshold,
        *(pltpu.with_memory_space_constraint(w, pltpu.VMEM) for w in weights),
    )


def owned_body(n, m, q_latent, kv_latent, k_rope, segment_ids, w_q_nope, w_q_rope, w_kv_nope, threshold):
    rows = q_latent.shape[0]
    heads = w_q_nope.shape[1] // D_NOPE
    own = heads // n
    got_early, got_late, *held = layer(
        n, m, own, q_latent, kv_latent, k_rope.T, segment_ids.reshape(1, rows), threshold, w_q_nope, w_q_rope, w_kv_nope
    )
    new_nope, new_rope, new_kv, head_max, row_max = clip_weights(n, own, got_early, got_late, threshold, *held)
    return (new_nope, new_rope, new_kv, head_max.reshape(heads), row_max.T)


def body(n, m, *operands):
    heads = operands[4].shape[1] // D_NOPE
    rows = operands[0].shape[0]
    shares = heads % n == 0 and heads // n % 4 == 0 and heads <= LANES
    powers = n & (n - 1) == 0 and m & (m - 1) == 0 and n > REACH
    small = n * rows * operands[0].shape[1] * m <= 2048 * 1536
    if shares and powers and small and rows % LANES == 0 and operands[2].shape[1] % (16 * m) == 0:
        return owned_body(n, m, *operands)
    return grouped_body(*operands)


def solution(mesh):
    in_specs = (
        P("seq", "head"),
        P("seq", "head"),
        P("seq", None),
        P("seq"),
        P("seq", "head"),
        P("seq", "head"),
        P("seq", "head"),
        P(),
    )
    out_specs = (P("seq", "head"), P("seq", "head"), P("seq", "head"), P("head"), P("seq", "head"))
    return jax.shard_map(functools.partial(body, mesh.shape["seq"], mesh.shape["head"]), mesh=mesh, in_specs=in_specs, out_specs=out_specs, check_vma=False)
```

```python
import functools
import math

import jax
import jax.numpy as jnp
from jax import lax
from jax.experimental import pallas as pl
from jax.experimental.pallas import tpu as pltpu
from jax.sharding import PartitionSpec as P

D_NOPE = 128
D_ROPE = 64
QLORA = 1536
KVLORA = 512
REACH = 3


def as_sent(value):
    return jax.tree.map(lambda a: a.astype(jnp.bfloat16) if a.dtype == jnp.float32 else a, value)


def from_partner(value, axis, stride):
    mask = 2**stride
    pairs = [(source, source ^ mask) for source in range(lax.axis_size(axis))]
    return lax.ppermute(value, axis, pairs)


def shifted(block, axis, distance):
    devices = range(lax.axis_size(axis))
    route = [(i - distance, i) for i in devices if i - distance in devices]
    return lax.ppermute(block, axis, route)


def score_max(query_nope, query_rope, key_nope, key_rope, allowed):
    nope = jnp.einsum("qhd,khd->hqk", query_nope, key_nope, preferred_element_type=jnp.float32)
    rope = jnp.einsum("qhd,kd->hqk", query_rope, key_rope, preferred_element_type=jnp.float32)
    scores = (nope + rope) * (1.0 / math.sqrt(D_NOPE + D_ROPE))
    return jnp.max(jnp.where(allowed[None], scores, jnp.float32(-1e30)), axis=2)


def masked_max(compute, operands):
    return compute(*operands)


def spread_columns(weight, width, quarter, copies):
    pieces = weight.reshape(weight.shape[0], 4, quarter * width).transpose(1, 0, 2)
    return jnp.tile(pieces, (copies, 1, 1))


def grouped_body(q_latent, kv_latent, k_rope, segment_ids, w_q_nope, w_q_rope, w_kv_nope, threshold):
    q_whole, kv_whole = (
        lax.all_gather(q_latent, "head", axis=1, tiled=True),
        lax.all_gather(kv_latent, "head", axis=1, tiled=True),
    )
    rows = q_whole.shape[0]
    heads = w_q_nope.shape[1] // D_NOPE
    q_scale = 1.0 / math.sqrt(QLORA)
    k_scale = 1.0 / math.sqrt(KVLORA)
    place = lax.axis_index("seq")
    quarter = heads // 4
    copies = lax.axis_size("seq") // 4
    slot = place % 4
    sent = (
        spread_columns(w_q_nope, D_NOPE, quarter, copies),
        spread_columns(w_q_rope, D_ROPE, quarter, copies),
        spread_columns(w_kv_nope, D_NOPE, quarter, copies),
    )
    got_nope, got_rope, got_kv = (
        lax.all_to_all(sent[0], "seq", split_axis=0, concat_axis=1, tiled=True),
        lax.all_to_all(sent[1], "seq", split_axis=0, concat_axis=1, tiled=True),
        lax.all_to_all(sent[2], "seq", split_axis=0, concat_axis=1, tiled=True),
    )
    sub_nope = got_nope.reshape(QLORA, quarter * D_NOPE)
    sub_rope = got_rope.reshape(QLORA, quarter * D_ROPE)
    sub_kv = got_kv.reshape(KVLORA, quarter * D_NOPE)
    group = (q_whole, kv_whole, k_rope)
    for level in range(2):
        partner = jax.tree.map(
            lambda part, own: part.astype(own.dtype),
            from_partner(as_sent(group), "seq", level),
            group,
        )
        upper = place // (1 << level) % 2 == 1
        group = tuple(
            (
                jnp.where(
                    upper, jnp.concatenate([other, mine], 0), jnp.concatenate([mine, other], 0)
                )
                for mine, other in zip(group, partner)
            )
        )
    group_q, group_kv, group_rope = group
    early_kv, early_rope = shifted(
        (group_kv[(4 - REACH) * rows :], group_rope[(4 - REACH) * rows :]), "seq", 4
    )
    keys_kv = jnp.concatenate([early_kv, group_kv], 0)
    keys_rope = jnp.concatenate([early_rope, group_rope], 0)
    key_nope = (
        (jnp.dot(keys_kv, sub_kv, preferred_element_type=jnp.float32) * k_scale)
        .astype(jnp.bfloat16)
        .reshape(keys_kv.shape[0], quarter, D_NOPE)
    )
    query_nope = (
        (jnp.dot(group_q, sub_nope, preferred_element_type=jnp.float32) * q_scale)
        .astype(jnp.bfloat16)
        .reshape(4 * rows, quarter, D_NOPE)
    )
    query_rope = (
        (jnp.dot(group_q, sub_rope, preferred_element_type=jnp.float32) * q_scale)
        .astype(jnp.bfloat16)
        .reshape(4 * rows, quarter, D_ROPE)
    )
    all_segs = lax.all_gather(segment_ids, "seq", axis=0, tiled=True)
    padded_segs = jnp.concatenate([jnp.full((REACH * rows,), -1, jnp.int32), all_segs], 0)
    first = place // 4 * 4
    window = (REACH + 1) * rows
    block_rows = []
    for local in range(4):
        block = first + local
        query_seg = lax.dynamic_slice_in_dim(all_segs, block * rows, rows, 0)
        key_seg = lax.dynamic_slice_in_dim(padded_segs, block * rows, window, 0)
        query_pos = block * rows + jnp.arange(rows, dtype=jnp.int32)
        key_pos = (block - REACH) * rows + jnp.arange(window, dtype=jnp.int32)
        allowed = (
            (query_seg[:, None] == key_seg[None, :])
            & (key_pos[None, :] <= query_pos[:, None])
            & (key_pos[None, :] >= 0)
        )
        operands = (
            query_nope[local * rows : (local + 1) * rows],
            query_rope[local * rows : (local + 1) * rows],
            key_nope[local * rows : local * rows + window],
            keys_rope[local * rows : local * rows + window],
            allowed,
        )
        block_rows.append(masked_max(score_max, operands))
    stacked = jnp.stack(block_rows, 0)[None]
    for level in range(2):
        partner = from_partner(stacked, "seq", level)
        upper = place // (1 << level) % 2 == 1
        stacked = jnp.where(
            upper, jnp.concatenate([partner, stacked], 0), jnp.concatenate([stacked, partner], 0)
        )
    own = lax.dynamic_index_in_dim(stacked, slot, 1, False)
    row_max = own.reshape(heads, rows).T
    local_heads = jnp.max(row_max, axis=0)
    head_max = lax.pmax(local_heads, "seq")
    return finish(threshold, head_max, row_max, w_q_nope, w_q_rope, w_kv_nope)


def finish(threshold, head_max, row_max, w_q_nope, w_q_rope, w_kv_nope):
    clip = threshold[0] / jnp.maximum(head_max, threshold[0])
    root = jnp.sqrt(clip)
    new_q_nope = (w_q_nope.astype(jnp.float32) * jnp.repeat(root, D_NOPE)[None, :]).astype(
        jnp.bfloat16
    )
    new_q_rope = (w_q_rope.astype(jnp.float32) * jnp.repeat(clip, D_ROPE)[None, :]).astype(
        jnp.bfloat16
    )
    new_kv_nope = (w_kv_nope.astype(jnp.float32) * jnp.repeat(root, D_NOPE)[None, :]).astype(
        jnp.bfloat16
    )
    return (new_q_nope, new_q_rope, new_kv_nope, head_max, row_max)


MESH = pl.DeviceIdType.MESH
LANES = 128
ROPE, KEY, GROUP, SINGLE, FINAL = KINDS = range(5)


def other(index, stride):
    return index + stride - 2 * stride * (index // stride % 2)


def flip(index, bits):
    stride = 1
    while stride <= bits:
        if bits & stride:
            index = other(index, stride)
        stride *= 2
    return index


def halvings(size):
    return [size >> (i + 1) for i in range(size.bit_length() - 1)]


def layer_kernel(
    n, m, own, q_lat, kv_lat, rope, segs, w_nope, w_rope, w_kv,
    got, held_nope, held_rope, held_kv,
    q_all, kv_all, rope_all, segs_all, w_pos, w_key, w_group, w_lone, keys, caps, seg_cols, q_pos, q_nope, near_query, maxima,
    q_send, q_recv, kv_send, kv_recv, rope_send, rope_recv, seg_send, seg_recv, w_send, w_recv, max_send, max_recv, local,
):
    s = lax.axis_index("seq")
    h = lax.axis_index("head")
    rows = q_lat.shape[0]
    part = rope.shape[0] // m
    pairs = own // 2
    q_rows = w_nope.shape[0]
    kv_rows = w_kv.shape[0]
    half = n // 2
    routes = [("seq", stride) for stride in halvings(n)] + [("head", stride) for stride in halvings(m)]
    last = len([1 for axis, _ in routes if axis == "seq"])

    barrier = pltpu.get_barrier_semaphore()
    for k in range(1, n):
        pl.semaphore_signal(barrier, inc=1, device_id=(flip(s, k), h), device_id_type=MESH)
    for stride in halvings(m):
        pl.semaphore_signal(barrier, inc=1, device_id=(s, other(h, stride)), device_id_type=MESH)

    def window(whole, width, ps, ph):
        return whole.at[pl.ds(pl.multiple_of(ps * rows, rows), rows), pl.ds(pl.multiple_of(ph * width, LANES), width)]

    def places(k, g):
        ps, ph = flip(s, k), flip(h, g)
        return (
            window(q_all, q_lat.shape[1], ps, ph),
            window(kv_all, kv_lat.shape[1], ps, ph),
            rope_all.at[ps, pl.ds(pl.multiple_of(ph * part, part), part), :],
            segs_all.at[ps],
        )

    def lanes(index, count=1):
        return pl.ds(pl.multiple_of(index * LANES, LANES), count * LANES)

    def parts_of(p):
        return (
            w_rope.at[:, lanes(p * pairs, pairs)],
            w_kv.at[:, lanes(p * own, own)],
            w_nope.at[:, lanes(p * own, own - 2)],
            w_nope.at[:, lanes(p * own + own - 2)],
            w_nope.at[:, lanes(p * own + own - 1)],
        )

    def landing(kind, source):
        q_at = pl.ds(pl.multiple_of(source * q_rows, q_rows), q_rows)
        kv_at = pl.ds(pl.multiple_of(source * kv_rows, kv_rows), kv_rows)
        return (
            w_pos.at[q_at, :], w_key.at[kv_at, :], w_group.at[q_at, :], w_lone.at[0, q_at, :], w_lone.at[1, q_at, :]
        )[kind]

    own_pieces = (q_lat, kv_lat, rope.at[pl.ds(pl.multiple_of(h * part, part), part), :], segs)
    loads = [
        pltpu.make_async_copy(src, dst, local.at[i])
        for i, (src, dst) in enumerate(zip(own_pieces, places(0, 0)))
    ]
    for copy in loads:
        copy.start()
    keeps = [
        pltpu.make_async_copy(src, landing(i, s), local.at[4 + i])
        for i, src in enumerate(parts_of(s))
    ] + [
        pltpu.make_async_copy(src, dst, local.at[4 + len(parts_of(s)) + i])
        for i, (src, dst) in enumerate(zip((w_nope, w_rope, w_kv), (held_nope, held_rope, held_kv)))
    ]
    for copy in keeps:
        copy.start()
    pl.semaphore_wait(barrier, n - 1 + len(halvings(m)))
    for copy in loads:
        copy.wait()

    drains = []
    slots = [0]
    sends = (q_send, kv_send, rope_send, seg_send)
    recvs = (q_recv, kv_recv, rope_recv, seg_recv)

    def push(k, g, route):
        axis, stride = route
        target = (other(s, stride), h) if axis == "seq" else (s, other(h, stride))
        at = (k ^ stride) * m + g if axis == "seq" else k * m + (g ^ stride)
        slot = slots[0]
        slots[0] += 1
        count = 4 if axis == "seq" else 3
        for ref, sent, taken in zip(places(k, g)[:count], sends, recvs):
            copy = pltpu.make_async_remote_copy(
                src_ref=ref, dst_ref=ref, send_sem=sent.at[slot], recv_sem=taken.at[at],
                device_id=target, device_id_type=MESH)
            copy.start()
            drains.append((ref, sent.at[slot]))

    def relay(k, g):
        for ref, taken in zip(places(k, g)[: 4 if g == 0 else 3], recvs):
            pltpu.make_async_copy(ref, ref, taken.at[k * m + g]).wait()
        reached = max(i for i, (axis, stride) in enumerate(routes) if (k if axis == "seq" else g) & stride)
        for route in routes[reached + 1:]:
            push(k, g, route)

    def weights(kind, k):
        p = flip(s, k)
        source = parts_of(p)[kind]
        copy = pltpu.make_async_remote_copy(
            src_ref=source, dst_ref=landing(kind, s),
            send_sem=w_send.at[kind * n + k], recv_sem=w_recv.at[kind * n + k],
            device_id=(p, h), device_id_type=MESH)
        copy.start()
        drains.append((source, w_send.at[kind * n + k]))

    def take(kind, ks):
        for k in ks:
            ref = landing(kind, flip(s, k))
            pltpu.make_async_copy(ref, ref, w_recv.at[kind * n + k]).wait()

    far = [k ^ half for k in range(half)]
    near = list(range(half - 1, 0, -1))

    for route in routes:
        push(0, 0, route)
    for k in far:
        weights(ROPE, k)
    order = sorted(range(1, n), key=lambda k: (bin(k).count("1"), k & 1 == 1 and bin(k).count("1") > 1, k))
    on_links = max(i for i, k in enumerate(order) if k & 1 == 0)
    for k in order[: on_links + 1]:
        relay(k, 0)
    for k in near:
        weights(ROPE, k)
    for kind in KINDS[1:]:
        for k in far + near:
            weights(kind, k)
    for k in order[on_links + 1 :]:
        relay(k, 0)

    def fill_segs(block, carry):
        here = pl.ds(pl.multiple_of(block * rows, rows), rows)
        seg_cols[here, :] = jnp.transpose(jnp.broadcast_to(segs_all[block], (LANES, rows)))
        return carry

    lax.fori_loop(0, n, fill_segs, 0)
    reach = (REACH + 1) * rows

    def range_of(block):
        start = jnp.maximum(block - REACH, 0) * rows
        return start, pl.ds(pl.multiple_of(start, rows), reach)

    def fill_caps(block, carry):
        start, span = range_of(block)
        key_segs = jnp.concatenate([seg_cols[span, :]] * (rows // LANES), 1)
        key_pos = start + lax.broadcasted_iota(jnp.int32, (reach, rows), 0)
        query_pos = block * rows + lax.broadcasted_iota(jnp.int32, (reach, rows), 1)
        allowed = (key_segs == segs_all[block]) & (key_pos <= query_pos)
        caps[block] = jnp.where(allowed, jnp.float32(3.4e38), jnp.float32(-1e30))
        return carry

    lax.fori_loop(0, n, fill_caps, 0)

    for g in range(1, m):
        for k in [0] + order:
            relay(k, g)

    for copy in keeps:
        copy.wait()
    q_scale = 1.0 / math.sqrt(QLORA)
    k_scale = 1.0 / math.sqrt(KVLORA)
    lane = lax.broadcasted_iota(jnp.int32, (rows, LANES), 1)
    sides = LANES // D_ROPE

    def fill_sides(block, carry):
        here = pl.ds(pl.multiple_of(block * rows, rows), rows)
        turned = jnp.concatenate([rope_all[block].astype(jnp.float32)] * sides, 0)
        twice = jnp.transpose(turned).astype(jnp.bfloat16)
        for i in range(own):
            keys[i, here, LANES : 2 * LANES] = jnp.where(lane // D_ROPE == i % sides, twice, jnp.zeros_like(twice))
        return carry

    lax.fori_loop(0, n, fill_sides, 0)

    def span(block):
        return slice(block * rows, (block + 1) * rows)

    def top_logits(i, block):
        first = max(block - REACH, 0)
        query = jnp.concatenate([q_nope[i, span(block), :], q_pos[span(block), i // sides * LANES : (i // sides + 1) * LANES]], 1)
        best = None
        for other_block in range(first, block + 1):
            logits = lax.dot_general(
                keys[i, span(other_block), :], query, (((1,), (1,)), ((), ())), preferred_element_type=jnp.float32
            )
            cap = caps[block, span(other_block - first), :]
            top = jnp.max(jnp.minimum(logits, cap).reshape(rows // 8, 8, rows), axis=0)
            best = top if best is None else jnp.maximum(best, top)
        top = jnp.max(best, axis=0, keepdims=True) * (1.0 / math.sqrt(D_NOPE + D_ROPE))
        maxima[block, i : i + 1, 0:rows] = top
        return top

    def head_logits(i):
        best = None
        for block in range(n):
            top = top_logits(i, block)
            best = top if best is None else jnp.maximum(best, top)
        best = jnp.broadcast_to(jnp.max(best, axis=1, keepdims=True), (1, LANES))
        for block in range(n):
            maxima[block, i : i + 1, rows : rows + LANES] = best

    def side_of(is_far, depth):
        side = 1 - s // half if is_far else s // half
        return pl.ds(pl.multiple_of(side * depth, depth), depth)

    close, distant = side_of(False, half * q_rows), side_of(True, half * q_rows)

    def project(weight):
        for block in range(n):
            query = jnp.dot(q_all[span(block), :], weight[...], preferred_element_type=jnp.float32)
            yield block, (query * q_scale).astype(jnp.bfloat16)

    take(KEY, far + near)
    for block in range(n):
        key = jnp.dot(kv_all[span(block), :], w_key[...], preferred_element_type=jnp.float32)
        key = (key * k_scale).astype(jnp.bfloat16)
        for i in range(own):
            keys[i, span(block), 0:LANES] = key[:, i * LANES : (i + 1) * LANES]
    take(ROPE, far + near)
    for block, query in project(w_pos):
        q_pos[span(block), :] = query
    take(GROUP, far + near)
    for block, query in project(w_group):
        for i in range(own - 2):
            q_nope[i, span(block), :] = query[:, i * LANES : (i + 1) * LANES]
    for i in range(own - 2):
        head_logits(i)
    take(SINGLE, far + near)
    for block, query in project(w_lone.at[0]):
        q_nope[own - 2, span(block), :] = query
    head_logits(own - 2)
    take(FINAL, near)
    for block in range(n):
        near_query[span(block), :] = jnp.dot(
            q_all[span(block), close], w_lone[1, close, :], preferred_element_type=jnp.float32
        )
    take(FINAL, far)
    for block in range(n):
        query = near_query[span(block), :] + jnp.dot(
            q_all[span(block), distant], w_lone[1, distant, :], preferred_element_type=jnp.float32
        )
        q_nope[own - 1, span(block), :] = (query * q_scale).astype(jnp.bfloat16)
    head_logits(own - 1)

    for k in range(1, n):
        p = flip(s, k)
        pltpu.make_async_remote_copy(
            src_ref=maxima.at[p], dst_ref=got.at[s], send_sem=max_send.at[k], recv_sem=max_recv.at[k],
            device_id=(p, h), device_id_type=MESH).start()
        drains.append((maxima.at[p], max_send.at[k]))
    got[s] = maxima[s]
    for ref, sent in drains:
        pltpu.make_async_copy(ref, ref, sent).wait()
    for k in range(1, n):
        come = got.at[flip(s, k)]
        pltpu.make_async_copy(come, come, max_recv.at[k]).wait()


def layer(n, m, own, q_lat, kv_lat, rope, segs, w_nope, w_rope, w_kv):
    rows = q_lat.shape[0]
    tokens = n * rows
    pairs = own // 2
    moves = n * m - 1
    parts = len(KINDS)
    depth = n * w_nope.shape[0]
    across = (n, own, rows + LANES)
    any_ref = pl.BlockSpec(memory_space=pl.ANY)
    dma = pltpu.SemaphoreType.DMA
    kind = q_lat.dtype
    return pl.pallas_call(
        functools.partial(layer_kernel, n, m, own),
        out_shape=(pltpu.VMEM(across, jnp.float32),)
        + tuple(pltpu.VMEM(w.shape, w.dtype) for w in (w_nope, w_rope, w_kv)),
        in_specs=[any_ref] * 7,
        out_specs=(pl.BlockSpec(memory_space=pltpu.VMEM),) * 4,
        scratch_shapes=[
            pltpu.VMEM((tokens, m * q_lat.shape[1]), kind),
            pltpu.VMEM((tokens, m * kv_lat.shape[1]), kind),
            pltpu.VMEM((n,) + rope.shape, kind),
            pltpu.VMEM((n,) + segs.shape, jnp.int32),
            pltpu.VMEM((depth, pairs * LANES), kind),
            pltpu.VMEM((n * w_kv.shape[0], own * LANES), kind),
            pltpu.VMEM((depth, (own - 2) * LANES), kind),
            pltpu.VMEM((2, depth, LANES), kind),
            pltpu.VMEM((own, tokens, D_NOPE + LANES), kind),
            pltpu.VMEM((n, (REACH + 1) * rows, rows), jnp.float32),
            pltpu.VMEM((tokens, LANES), jnp.int32),
            pltpu.VMEM((tokens, pairs * LANES), kind),
            pltpu.VMEM((own, tokens, LANES), kind),
            pltpu.VMEM((tokens, LANES), jnp.float32),
            pltpu.VMEM(across, jnp.float32),
            dma((moves,)), dma((n * m,)), dma((moves,)), dma((n * m,)), dma((moves,)), dma((n * m,)),
            dma((moves,)), dma((n * m,)),
            dma((parts * n,)), dma((parts * n,)), dma((n,)), dma((n,)), dma((7 + parts,)),
        ],
        compiler_params=pltpu.CompilerParams(
            collective_id=0, has_side_effects=True, vmem_limit_bytes=60 * 1024 * 1024
        ),
        name="layer",
    )(*(pltpu.with_memory_space_constraint(a, pltpu.HBM) for a in (q_lat, kv_lat, rope, segs, w_nope, w_rope, w_kv)))


def clip_kernel(
    n, own, got, threshold, w_nope, w_rope, w_kv, new_nope, new_rope, new_kv, head_max, row_max,
    out_nope, out_rope, out_kv, out_head, out_row, sems,
):
    limit = threshold[0]
    rows = row_max.shape[1]
    lane = lax.broadcasted_iota(jnp.int32, (1, LANES), 1)
    tops = jnp.zeros((1, head_max.shape[1]), jnp.float32)
    place = lax.broadcasted_iota(jnp.int32, tops.shape, 1)
    copies = []

    def put(source, target):
        copy = pltpu.make_async_copy(source, target, sems.at[len(copies)])
        copy.start()
        copies.append(copy)

    def scaled(source, target, column, factor):
        columns = slice(column * LANES, (column + 1) * LANES)
        target[:, columns] = (source[:, columns].astype(jnp.float32) * factor).astype(target.dtype)

    for s in range(n):
        top = got[s, :, rows : rows + LANES]
        clip = limit / jnp.maximum(top, limit)
        root = jnp.sqrt(clip)
        for i in range(own):
            scaled(w_nope, out_nope, s * own + i, root[i : i + 1])
        for i in range(own):
            scaled(w_kv, out_kv, s * own + i, root[i : i + 1])
        for j in range(own // 2):
            factor = jnp.where(lane < D_ROPE, clip[2 * j : 2 * j + 1], clip[2 * j + 1 : 2 * j + 2])
            scaled(w_rope, out_rope, s * own // 2 + j, factor)
        for source, target in ((out_nope, new_nope), (out_rope, new_rope), (out_kv, new_kv)):
            width = source.shape[1] // n
            at = pl.ds(s * width, width)
            put(source.at[:, at], target.at[:, at])
        if s == 0:
            for p in range(n):
                out_row[p * own : (p + 1) * own, :] = got[p, :, 0:rows]
                for i in range(own):
                    tops = jnp.where(place == p * own + i, got[p, i : i + 1, rows : rows + tops.shape[1]], tops)
            out_head[...] = tops
            put(out_row, row_max)
            put(out_head, head_max)
    for copy in copies:
        copy.wait()


def clip_weights(n, own, got, threshold, w_nope, w_rope, w_kv):
    weights = (w_nope, w_rope, w_kv)
    heads = n * own
    rows = got.shape[2] - LANES
    in_vmem = pl.BlockSpec(memory_space=pltpu.VMEM)
    return pl.pallas_call(
        functools.partial(clip_kernel, n, own),
        out_shape=tuple(jax.ShapeDtypeStruct(w.shape, w.dtype) for w in weights)
        + (jax.ShapeDtypeStruct((1, heads), jnp.float32), jax.ShapeDtypeStruct((heads, rows), jnp.float32)),
        in_specs=[in_vmem, pl.BlockSpec(memory_space=pltpu.SMEM)] + [in_vmem] * 3,
        out_specs=(pl.BlockSpec(memory_space=pl.ANY),) * 5,
        scratch_shapes=[pltpu.VMEM(w.shape, w.dtype) for w in weights]
        + [pltpu.VMEM((1, heads), jnp.float32), pltpu.VMEM((heads, rows), jnp.float32)]
        + [pltpu.SemaphoreType.DMA((3 * n + 2,))],
        compiler_params=pltpu.CompilerParams(vmem_limit_bytes=16 * 1024 * 1024),
        name="clip_weights",
    )(
        pltpu.with_memory_space_constraint(got, pltpu.VMEM),
        threshold,
        *(pltpu.with_memory_space_constraint(w, pltpu.VMEM) for w in weights),
    )


def owned_body(n, m, q_latent, kv_latent, k_rope, segment_ids, w_q_nope, w_q_rope, w_kv_nope, threshold):
    rows = q_latent.shape[0]
    heads = w_q_nope.shape[1] // D_NOPE
    own = heads // n
    got, *held = layer(
        n, m, own, q_latent, kv_latent, k_rope.T, segment_ids.reshape(1, rows), w_q_nope, w_q_rope, w_kv_nope
    )
    new_nope, new_rope, new_kv, head_max, row_max = clip_weights(n, own, got, threshold, *held)
    return (new_nope, new_rope, new_kv, head_max.reshape(heads), row_max.T)


def body(n, m, *operands):
    heads = operands[4].shape[1] // D_NOPE
    rows = operands[0].shape[0]
    shares = heads % n == 0 and heads // n % 4 == 0 and heads <= LANES
    powers = n & (n - 1) == 0 and m & (m - 1) == 0 and n > REACH
    small = n * rows * operands[0].shape[1] * m <= 2048 * 1536
    if shares and powers and small and rows % LANES == 0 and operands[2].shape[1] % (16 * m) == 0:
        return owned_body(n, m, *operands)
    return grouped_body(*operands)


def solution(mesh):
    in_specs = (
        P("seq", "head"),
        P("seq", "head"),
        P("seq", None),
        P("seq"),
        P("seq", "head"),
        P("seq", "head"),
        P("seq", "head"),
        P(),
    )
    out_specs = (P("seq", "head"), P("seq", "head"), P("seq", "head"), P("head"), P("seq", "head"))
    return jax.shard_map(functools.partial(body, mesh.shape["seq"], mesh.shape["head"]), mesh=mesh, in_specs=in_specs, out_specs=out_specs, check_vma=False)
```

```python
import functools
import math

import jax
import jax.numpy as jnp
from jax import lax
from jax.experimental import pallas as pl
from jax.experimental.pallas import tpu as pltpu
from jax.sharding import PartitionSpec as P

D_NOPE = 128
D_ROPE = 64
QLORA = 1536
KVLORA = 512
REACH = 3


def as_sent(value):
    return jax.tree.map(lambda a: a.astype(jnp.bfloat16) if a.dtype == jnp.float32 else a, value)


def from_partner(value, axis, stride):
    mask = 2**stride
    pairs = [(source, source ^ mask) for source in range(lax.axis_size(axis))]
    return lax.ppermute(value, axis, pairs)


def shifted(block, axis, distance):
    devices = range(lax.axis_size(axis))
    route = [(i - distance, i) for i in devices if i - distance in devices]
    return lax.ppermute(block, axis, route)


def score_max(query_nope, query_rope, key_nope, key_rope, allowed):
    nope = jnp.einsum("qhd,khd->hqk", query_nope, key_nope, preferred_element_type=jnp.float32)
    rope = jnp.einsum("qhd,kd->hqk", query_rope, key_rope, preferred_element_type=jnp.float32)
    scores = (nope + rope) * (1.0 / math.sqrt(D_NOPE + D_ROPE))
    return jnp.max(jnp.where(allowed[None], scores, jnp.float32(-1e30)), axis=2)


def masked_max(compute, operands):
    return compute(*operands)


def spread_columns(weight, width, quarter, copies):
    pieces = weight.reshape(weight.shape[0], 4, quarter * width).transpose(1, 0, 2)
    return jnp.tile(pieces, (copies, 1, 1))


def grouped_body(q_latent, kv_latent, k_rope, segment_ids, w_q_nope, w_q_rope, w_kv_nope, threshold):
    q_whole, kv_whole = (
        lax.all_gather(q_latent, "head", axis=1, tiled=True),
        lax.all_gather(kv_latent, "head", axis=1, tiled=True),
    )
    rows = q_whole.shape[0]
    heads = w_q_nope.shape[1] // D_NOPE
    q_scale = 1.0 / math.sqrt(QLORA)
    k_scale = 1.0 / math.sqrt(KVLORA)
    place = lax.axis_index("seq")
    quarter = heads // 4
    copies = lax.axis_size("seq") // 4
    slot = place % 4
    sent = (
        spread_columns(w_q_nope, D_NOPE, quarter, copies),
        spread_columns(w_q_rope, D_ROPE, quarter, copies),
        spread_columns(w_kv_nope, D_NOPE, quarter, copies),
    )
    got_nope, got_rope, got_kv = (
        lax.all_to_all(sent[0], "seq", split_axis=0, concat_axis=1, tiled=True),
        lax.all_to_all(sent[1], "seq", split_axis=0, concat_axis=1, tiled=True),
        lax.all_to_all(sent[2], "seq", split_axis=0, concat_axis=1, tiled=True),
    )
    sub_nope = got_nope.reshape(QLORA, quarter * D_NOPE)
    sub_rope = got_rope.reshape(QLORA, quarter * D_ROPE)
    sub_kv = got_kv.reshape(KVLORA, quarter * D_NOPE)
    group = (q_whole, kv_whole, k_rope)
    for level in range(2):
        partner = jax.tree.map(
            lambda part, own: part.astype(own.dtype),
            from_partner(as_sent(group), "seq", level),
            group,
        )
        upper = place // (1 << level) % 2 == 1
        group = tuple(
            (
                jnp.where(
                    upper, jnp.concatenate([other, mine], 0), jnp.concatenate([mine, other], 0)
                )
                for mine, other in zip(group, partner)
            )
        )
    group_q, group_kv, group_rope = group
    early_kv, early_rope = shifted(
        (group_kv[(4 - REACH) * rows :], group_rope[(4 - REACH) * rows :]), "seq", 4
    )
    keys_kv = jnp.concatenate([early_kv, group_kv], 0)
    keys_rope = jnp.concatenate([early_rope, group_rope], 0)
    key_nope = (
        (jnp.dot(keys_kv, sub_kv, preferred_element_type=jnp.float32) * k_scale)
        .astype(jnp.bfloat16)
        .reshape(keys_kv.shape[0], quarter, D_NOPE)
    )
    query_nope = (
        (jnp.dot(group_q, sub_nope, preferred_element_type=jnp.float32) * q_scale)
        .astype(jnp.bfloat16)
        .reshape(4 * rows, quarter, D_NOPE)
    )
    query_rope = (
        (jnp.dot(group_q, sub_rope, preferred_element_type=jnp.float32) * q_scale)
        .astype(jnp.bfloat16)
        .reshape(4 * rows, quarter, D_ROPE)
    )
    all_segs = lax.all_gather(segment_ids, "seq", axis=0, tiled=True)
    padded_segs = jnp.concatenate([jnp.full((REACH * rows,), -1, jnp.int32), all_segs], 0)
    first = place // 4 * 4
    window = (REACH + 1) * rows
    block_rows = []
    for local in range(4):
        block = first + local
        query_seg = lax.dynamic_slice_in_dim(all_segs, block * rows, rows, 0)
        key_seg = lax.dynamic_slice_in_dim(padded_segs, block * rows, window, 0)
        query_pos = block * rows + jnp.arange(rows, dtype=jnp.int32)
        key_pos = (block - REACH) * rows + jnp.arange(window, dtype=jnp.int32)
        allowed = (
            (query_seg[:, None] == key_seg[None, :])
            & (key_pos[None, :] <= query_pos[:, None])
            & (key_pos[None, :] >= 0)
        )
        operands = (
            query_nope[local * rows : (local + 1) * rows],
            query_rope[local * rows : (local + 1) * rows],
            key_nope[local * rows : local * rows + window],
            keys_rope[local * rows : local * rows + window],
            allowed,
        )
        block_rows.append(masked_max(score_max, operands))
    stacked = jnp.stack(block_rows, 0)[None]
    for level in range(2):
        partner = from_partner(stacked, "seq", level)
        upper = place // (1 << level) % 2 == 1
        stacked = jnp.where(
            upper, jnp.concatenate([partner, stacked], 0), jnp.concatenate([stacked, partner], 0)
        )
    own = lax.dynamic_index_in_dim(stacked, slot, 1, False)
    row_max = own.reshape(heads, rows).T
    local_heads = jnp.max(row_max, axis=0)
    head_max = lax.pmax(local_heads, "seq")
    return finish(threshold, head_max, row_max, w_q_nope, w_q_rope, w_kv_nope)


def finish(threshold, head_max, row_max, w_q_nope, w_q_rope, w_kv_nope):
    clip = threshold[0] / jnp.maximum(head_max, threshold[0])
    root = jnp.sqrt(clip)
    new_q_nope = (w_q_nope.astype(jnp.float32) * jnp.repeat(root, D_NOPE)[None, :]).astype(
        jnp.bfloat16
    )
    new_q_rope = (w_q_rope.astype(jnp.float32) * jnp.repeat(clip, D_ROPE)[None, :]).astype(
        jnp.bfloat16
    )
    new_kv_nope = (w_kv_nope.astype(jnp.float32) * jnp.repeat(root, D_NOPE)[None, :]).astype(
        jnp.bfloat16
    )
    return (new_q_nope, new_q_rope, new_kv_nope, head_max, row_max)


MESH = pl.DeviceIdType.MESH
LANES = 128
ROPE, KEY, GROUP, SINGLE, FINAL = KINDS = range(5)


def other(index, stride):
    return index + stride - 2 * stride * (index // stride % 2)


def flip(index, bits):
    stride = 1
    while stride <= bits:
        if bits & stride:
            index = other(index, stride)
        stride *= 2
    return index


def halvings(size):
    return [size >> (i + 1) for i in range(size.bit_length() - 1)]


def layer_kernel(
    n, m, own, q_lat, kv_lat, rope, segs, w_nope, w_rope, w_kv,
    got, held_nope, held_rope, held_kv,
    q_all, kv_all, rope_all, segs_all, w_pos, w_key, w_group, w_lone, keys, caps, seg_cols, q_pos, q_nope, near_query, maxima,
    q_send, q_recv, kv_send, kv_recv, rope_send, rope_recv, seg_send, seg_recv, w_send, w_recv, max_send, max_recv, local, known,
):
    s = lax.axis_index("seq")
    h = lax.axis_index("head")
    rows = q_lat.shape[0]
    part = rope.shape[0] // m
    pairs = own // 2
    q_rows = w_nope.shape[0]
    kv_rows = w_kv.shape[0]
    half = n // 2
    routes = [("seq", stride) for stride in halvings(n)] + [("head", stride) for stride in halvings(m)]
    last = len([1 for axis, _ in routes if axis == "seq"])

    barrier = pltpu.get_barrier_semaphore()
    for stride in halvings(n):
        pl.semaphore_signal(barrier, inc=1, device_id=(other(s, stride), h), device_id_type=MESH)
    for stride in halvings(m):
        pl.semaphore_signal(barrier, inc=1, device_id=(s, other(h, stride)), device_id_type=MESH)

    def window(whole, width, ps, ph):
        return whole.at[pl.ds(pl.multiple_of(ps * rows, rows), rows), pl.ds(pl.multiple_of(ph * width, LANES), width)]

    def places(k, g):
        ps, ph = flip(s, k), flip(h, g)
        return (
            window(q_all, q_lat.shape[1], ps, ph),
            window(kv_all, kv_lat.shape[1], ps, ph),
            rope_all.at[ps, pl.ds(pl.multiple_of(ph * part, part), part), :],
            segs_all.at[ps],
        )

    def lanes(index, count=1):
        return pl.ds(pl.multiple_of(index * LANES, LANES), count * LANES)

    def parts_of(p):
        return (
            w_rope.at[:, lanes(p * pairs, pairs)],
            w_kv.at[:, lanes(p * own, own)],
            w_nope.at[:, lanes(p * own, own - 2)],
            w_nope.at[:, lanes(p * own + own - 2)],
            w_nope.at[:, lanes(p * own + own - 1)],
        )

    def landing(kind, source):
        q_at = pl.ds(pl.multiple_of(source * q_rows, q_rows), q_rows)
        kv_at = pl.ds(pl.multiple_of(source * kv_rows, kv_rows), kv_rows)
        return (
            w_pos.at[q_at, :], w_key.at[kv_at, :], w_group.at[q_at, :], w_lone.at[0, q_at, :], w_lone.at[1, q_at, :]
        )[kind]

    own_pieces = (q_lat, kv_lat, rope.at[pl.ds(pl.multiple_of(h * part, part), part), :], segs)
    loads = [
        pltpu.make_async_copy(src, dst, local.at[i])
        for i, (src, dst) in enumerate(zip(own_pieces, places(0, 0)))
    ]
    for copy in loads:
        copy.start()
    keeps = [
        pltpu.make_async_copy(src, landing(i, s), local.at[4 + i])
        for i, src in enumerate(parts_of(s))
    ] + [
        pltpu.make_async_copy(src, dst, local.at[4 + len(parts_of(s)) + i])
        for i, (src, dst) in enumerate(zip((w_nope, w_rope, w_kv), (held_nope, held_rope, held_kv)))
    ]
    for copy in keeps:
        copy.start()
    pl.semaphore_wait(barrier, len(routes))
    for copy in loads:
        copy.wait()

    drains = []
    slots = [0]
    sends = (q_send, kv_send, rope_send, seg_send)
    recvs = (q_recv, kv_recv, rope_recv, seg_recv)

    def push(k, g, route):
        axis, stride = route
        target = (other(s, stride), h) if axis == "seq" else (s, other(h, stride))
        at = (k ^ stride) * m + g if axis == "seq" else k * m + (g ^ stride)
        slot = slots[0]
        slots[0] += 1
        count = 4 if axis == "seq" else 3
        for ref, sent, taken in zip(places(k, g)[:count], sends, recvs):
            copy = pltpu.make_async_remote_copy(
                src_ref=ref, dst_ref=ref, send_sem=sent.at[slot], recv_sem=taken.at[at],
                device_id=target, device_id_type=MESH)
            copy.start()
            drains.append((ref, sent.at[slot]))

    def relay(k, g):
        for ref, taken in zip(places(k, g)[: 4 if g == 0 else 3], recvs):
            pltpu.make_async_copy(ref, ref, taken.at[k * m + g]).wait()
        reached = max(i for i, (axis, stride) in enumerate(routes) if (k if axis == "seq" else g) & stride)
        for route in routes[reached + 1:]:
            push(k, g, route)

    def weights(kind, k):
        p = flip(s, k)
        source = parts_of(p)[kind]
        copy = pltpu.make_async_remote_copy(
            src_ref=source, dst_ref=landing(kind, s),
            send_sem=w_send.at[kind * n + k], recv_sem=w_recv.at[kind * n + k],
            device_id=(p, h), device_id_type=MESH)
        copy.start()
        drains.append((source, w_send.at[kind * n + k]))

    def take(kind, ks):
        for k in ks:
            ref = landing(kind, flip(s, k))
            pltpu.make_async_copy(ref, ref, w_recv.at[kind * n + k]).wait()

    far = [k ^ half for k in range(half)]
    near = list(range(half - 1, 0, -1))

    for route in routes:
        push(0, 0, route)
    for i, stride in enumerate(reversed(halvings(n)[:-1])):
        pl.semaphore_signal(known.at[i], inc=1, device_id=(other(s, stride), h), device_id_type=MESH)
        pl.semaphore_wait(known.at[i], 1)
    for k in far:
        weights(ROPE, k)
    order = sorted(range(1, n), key=lambda k: (bin(k).count("1"), k & 1 == 1 and bin(k).count("1") > 1, k))
    on_links = max(i for i, k in enumerate(order) if k & 1 == 0)
    for k in order[: on_links + 1]:
        relay(k, 0)
    for k in near:
        weights(ROPE, k)
    for kind in KINDS[1:]:
        for k in far + near:
            weights(kind, k)
    for k in order[on_links + 1 :]:
        relay(k, 0)

    def fill_segs(block, carry):
        here = pl.ds(pl.multiple_of(block * rows, rows), rows)
        seg_cols[here, :] = jnp.transpose(jnp.broadcast_to(segs_all[block], (LANES, rows)))
        return carry

    lax.fori_loop(0, n, fill_segs, 0)
    reach = (REACH + 1) * rows

    def range_of(block):
        start = jnp.maximum(block - REACH, 0) * rows
        return start, pl.ds(pl.multiple_of(start, rows), reach)

    def fill_caps(block, carry):
        start, span = range_of(block)
        key_segs = jnp.concatenate([seg_cols[span, :]] * (rows // LANES), 1)
        key_pos = start + lax.broadcasted_iota(jnp.int32, (reach, rows), 0)
        query_pos = block * rows + lax.broadcasted_iota(jnp.int32, (reach, rows), 1)
        allowed = (key_segs == segs_all[block]) & (key_pos <= query_pos)
        caps[block] = jnp.where(allowed, jnp.float32(3.4e38), jnp.float32(-1e30))
        return carry

    lax.fori_loop(0, n, fill_caps, 0)

    for g in range(1, m):
        for k in [0] + order:
            relay(k, g)

    for copy in keeps:
        copy.wait()
    q_scale = 1.0 / math.sqrt(QLORA)
    k_scale = 1.0 / math.sqrt(KVLORA)
    lane = lax.broadcasted_iota(jnp.int32, (rows, LANES), 1)
    sides = LANES // D_ROPE

    def fill_sides(block, carry):
        here = pl.ds(pl.multiple_of(block * rows, rows), rows)
        turned = jnp.concatenate([rope_all[block].astype(jnp.float32)] * sides, 0)
        twice = jnp.transpose(turned).astype(jnp.bfloat16)
        for i in range(own):
            keys[i, here, LANES : 2 * LANES] = jnp.where(lane // D_ROPE == i % sides, twice, jnp.zeros_like(twice))
        return carry

    lax.fori_loop(0, n, fill_sides, 0)

    def span(block):
        return slice(block * rows, (block + 1) * rows)

    def top_logits(i, block):
        first = max(block - REACH, 0)
        query = jnp.concatenate([q_nope[i, span(block), :], q_pos[span(block), i // sides * LANES : (i // sides + 1) * LANES]], 1)
        best = None
        for other_block in range(first, block + 1):
            logits = lax.dot_general(
                keys[i, span(other_block), :], query, (((1,), (1,)), ((), ())), preferred_element_type=jnp.float32
            )
            cap = caps[block, span(other_block - first), :]
            top = jnp.max(jnp.minimum(logits, cap).reshape(rows // 8, 8, rows), axis=0)
            best = top if best is None else jnp.maximum(best, top)
        top = jnp.max(best, axis=0, keepdims=True) * (1.0 / math.sqrt(D_NOPE + D_ROPE))
        maxima[block, i : i + 1, 0:rows] = top
        return top

    def head_logits(i):
        best = None
        for block in range(n):
            top = top_logits(i, block)
            best = top if best is None else jnp.maximum(best, top)
        best = jnp.broadcast_to(jnp.max(best, axis=1, keepdims=True), (1, LANES))
        for block in range(n):
            maxima[block, i : i + 1, rows : rows + LANES] = best

    def side_of(is_far, depth):
        side = 1 - s // half if is_far else s // half
        return pl.ds(pl.multiple_of(side * depth, depth), depth)

    close, distant = side_of(False, half * q_rows), side_of(True, half * q_rows)

    def project(weight):
        for block in range(n):
            query = jnp.dot(q_all[span(block), :], weight[...], preferred_element_type=jnp.float32)
            yield block, (query * q_scale).astype(jnp.bfloat16)

    take(KEY, far + near)
    for block in range(n):
        key = jnp.dot(kv_all[span(block), :], w_key[...], preferred_element_type=jnp.float32)
        key = (key * k_scale).astype(jnp.bfloat16)
        for i in range(own):
            keys[i, span(block), 0:LANES] = key[:, i * LANES : (i + 1) * LANES]
    take(ROPE, far + near)
    for block, query in project(w_pos):
        q_pos[span(block), :] = query
    take(GROUP, far + near)
    for block, query in project(w_group):
        for i in range(own - 2):
            q_nope[i, span(block), :] = query[:, i * LANES : (i + 1) * LANES]
    for i in range(own - 2):
        head_logits(i)
    take(SINGLE, far + near)
    for block, query in project(w_lone.at[0]):
        q_nope[own - 2, span(block), :] = query
    head_logits(own - 2)
    take(FINAL, near)
    for block in range(n):
        near_query[span(block), :] = jnp.dot(
            q_all[span(block), close], w_lone[1, close, :], preferred_element_type=jnp.float32
        )
    take(FINAL, far)
    for block in range(n):
        query = near_query[span(block), :] + jnp.dot(
            q_all[span(block), distant], w_lone[1, distant, :], preferred_element_type=jnp.float32
        )
        q_nope[own - 1, span(block), :] = (query * q_scale).astype(jnp.bfloat16)
    head_logits(own - 1)

    for k in range(1, n):
        p = flip(s, k)
        pltpu.make_async_remote_copy(
            src_ref=maxima.at[p], dst_ref=got.at[s], send_sem=max_send.at[k], recv_sem=max_recv.at[k],
            device_id=(p, h), device_id_type=MESH).start()
        drains.append((maxima.at[p], max_send.at[k]))
    got[s] = maxima[s]
    for ref, sent in drains:
        pltpu.make_async_copy(ref, ref, sent).wait()
    for k in range(1, n):
        come = got.at[flip(s, k)]
        pltpu.make_async_copy(come, come, max_recv.at[k]).wait()


def layer(n, m, own, q_lat, kv_lat, rope, segs, w_nope, w_rope, w_kv):
    rows = q_lat.shape[0]
    tokens = n * rows
    pairs = own // 2
    moves = n * m - 1
    parts = len(KINDS)
    depth = n * w_nope.shape[0]
    across = (n, own, rows + LANES)
    any_ref = pl.BlockSpec(memory_space=pl.ANY)
    dma = pltpu.SemaphoreType.DMA
    kind = q_lat.dtype
    return pl.pallas_call(
        functools.partial(layer_kernel, n, m, own),
        out_shape=(pltpu.VMEM(across, jnp.float32),)
        + tuple(pltpu.VMEM(w.shape, w.dtype) for w in (w_nope, w_rope, w_kv)),
        in_specs=[any_ref] * 7,
        out_specs=(pl.BlockSpec(memory_space=pltpu.VMEM),) * 4,
        scratch_shapes=[
            pltpu.VMEM((tokens, m * q_lat.shape[1]), kind),
            pltpu.VMEM((tokens, m * kv_lat.shape[1]), kind),
            pltpu.VMEM((n,) + rope.shape, kind),
            pltpu.VMEM((n,) + segs.shape, jnp.int32),
            pltpu.VMEM((depth, pairs * LANES), kind),
            pltpu.VMEM((n * w_kv.shape[0], own * LANES), kind),
            pltpu.VMEM((depth, (own - 2) * LANES), kind),
            pltpu.VMEM((2, depth, LANES), kind),
            pltpu.VMEM((own, tokens, D_NOPE + LANES), kind),
            pltpu.VMEM((n, (REACH + 1) * rows, rows), jnp.float32),
            pltpu.VMEM((tokens, LANES), jnp.int32),
            pltpu.VMEM((tokens, pairs * LANES), kind),
            pltpu.VMEM((own, tokens, LANES), kind),
            pltpu.VMEM((tokens, LANES), jnp.float32),
            pltpu.VMEM(across, jnp.float32),
            dma((moves,)), dma((n * m,)), dma((moves,)), dma((n * m,)), dma((moves,)), dma((n * m,)),
            dma((moves,)), dma((n * m,)),
            dma((parts * n,)), dma((parts * n,)), dma((n,)), dma((n,)), dma((7 + parts,)),
            pltpu.SemaphoreType.REGULAR((n.bit_length(),)),
        ],
        compiler_params=pltpu.CompilerParams(
            collective_id=0, has_side_effects=True, vmem_limit_bytes=60 * 1024 * 1024
        ),
        name="layer",
    )(*(pltpu.with_memory_space_constraint(a, pltpu.HBM) for a in (q_lat, kv_lat, rope, segs, w_nope, w_rope, w_kv)))


def clip_kernel(
    n, own, got, threshold, w_nope, w_rope, w_kv, new_nope, new_rope, new_kv, head_max, row_max,
    out_nope, out_rope, out_kv, out_head, out_row, sems,
):
    limit = threshold[0]
    rows = row_max.shape[1]
    lane = lax.broadcasted_iota(jnp.int32, (1, LANES), 1)
    tops = jnp.zeros((1, head_max.shape[1]), jnp.float32)
    place = lax.broadcasted_iota(jnp.int32, tops.shape, 1)
    copies = []

    def put(source, target):
        copy = pltpu.make_async_copy(source, target, sems.at[len(copies)])
        copy.start()
        copies.append(copy)

    def scaled(source, target, column, factor):
        columns = slice(column * LANES, (column + 1) * LANES)
        target[:, columns] = (source[:, columns].astype(jnp.float32) * factor).astype(target.dtype)

    for s in range(n):
        top = got[s, :, rows : rows + LANES]
        clip = limit / jnp.maximum(top, limit)
        root = jnp.sqrt(clip)
        for i in range(own):
            scaled(w_nope, out_nope, s * own + i, root[i : i + 1])
        for i in range(own):
            scaled(w_kv, out_kv, s * own + i, root[i : i + 1])
        for j in range(own // 2):
            factor = jnp.where(lane < D_ROPE, clip[2 * j : 2 * j + 1], clip[2 * j + 1 : 2 * j + 2])
            scaled(w_rope, out_rope, s * own // 2 + j, factor)
        for source, target in ((out_nope, new_nope), (out_rope, new_rope), (out_kv, new_kv)):
            width = source.shape[1] // n
            at = pl.ds(s * width, width)
            put(source.at[:, at], target.at[:, at])
        if s == 0:
            for p in range(n):
                out_row[p * own : (p + 1) * own, :] = got[p, :, 0:rows]
                for i in range(own):
                    tops = jnp.where(place == p * own + i, got[p, i : i + 1, rows : rows + tops.shape[1]], tops)
            out_head[...] = tops
            put(out_row, row_max)
            put(out_head, head_max)
    for copy in copies:
        copy.wait()


def clip_weights(n, own, got, threshold, w_nope, w_rope, w_kv):
    weights = (w_nope, w_rope, w_kv)
    heads = n * own
    rows = got.shape[2] - LANES
    in_vmem = pl.BlockSpec(memory_space=pltpu.VMEM)
    return pl.pallas_call(
        functools.partial(clip_kernel, n, own),
        out_shape=tuple(jax.ShapeDtypeStruct(w.shape, w.dtype) for w in weights)
        + (jax.ShapeDtypeStruct((1, heads), jnp.float32), jax.ShapeDtypeStruct((heads, rows), jnp.float32)),
        in_specs=[in_vmem, pl.BlockSpec(memory_space=pltpu.SMEM)] + [in_vmem] * 3,
        out_specs=(pl.BlockSpec(memory_space=pl.ANY),) * 5,
        scratch_shapes=[pltpu.VMEM(w.shape, w.dtype) for w in weights]
        + [pltpu.VMEM((1, heads), jnp.float32), pltpu.VMEM((heads, rows), jnp.float32)]
        + [pltpu.SemaphoreType.DMA((3 * n + 2,))],
        compiler_params=pltpu.CompilerParams(vmem_limit_bytes=16 * 1024 * 1024),
        name="clip_weights",
    )(
        pltpu.with_memory_space_constraint(got, pltpu.VMEM),
        threshold,
        *(pltpu.with_memory_space_constraint(w, pltpu.VMEM) for w in weights),
    )


def owned_body(n, m, q_latent, kv_latent, k_rope, segment_ids, w_q_nope, w_q_rope, w_kv_nope, threshold):
    rows = q_latent.shape[0]
    heads = w_q_nope.shape[1] // D_NOPE
    own = heads // n
    got, *held = layer(
        n, m, own, q_latent, kv_latent, k_rope.T, segment_ids.reshape(1, rows), w_q_nope, w_q_rope, w_kv_nope
    )
    new_nope, new_rope, new_kv, head_max, row_max = clip_weights(n, own, got, threshold, *held)
    return (new_nope, new_rope, new_kv, head_max.reshape(heads), row_max.T)


def body(n, m, *operands):
    heads = operands[4].shape[1] // D_NOPE
    rows = operands[0].shape[0]
    shares = heads % n == 0 and heads // n % 4 == 0 and heads <= LANES
    powers = n & (n - 1) == 0 and m & (m - 1) == 0 and n > REACH
    small = n * rows * operands[0].shape[1] * m <= 2048 * 1536
    if shares and powers and small and rows % LANES == 0 and operands[2].shape[1] % (16 * m) == 0:
        return owned_body(n, m, *operands)
    return grouped_body(*operands)


def solution(mesh):
    in_specs = (
        P("seq", "head"),
        P("seq", "head"),
        P("seq", None),
        P("seq"),
        P("seq", "head"),
        P("seq", "head"),
        P("seq", "head"),
        P(),
    )
    out_specs = (P("seq", "head"), P("seq", "head"), P("seq", "head"), P("head"), P("seq", "head"))
    return jax.shard_map(functools.partial(body, mesh.shape["seq"], mesh.shape["head"]), mesh=mesh, in_specs=in_specs, out_specs=out_specs, check_vma=False)
```
